8 devices in a mesh: data: 2 (over z, y), pair: 4 (over x, core).
Axes of the slice: x: 2, y: 2, z: 1, core: 2. Of those that a mesh axis runs over, the one named last changes fastest.
Arguments:
- x_enc: bfloat16 [256, 256, 1024], P(('data', 'pair')), parts along dimension 0
- enc_len: int32 [256], P(('data', 'pair')), parts along dimension 0
- y_dec: bfloat16 [256, 96, 1024], P(('data', 'pair')), parts along dimension 0
- enc_wq: bfloat16 [2, 1024, 1024], replicated
- enc_wk: bfloat16 [2, 1024, 1024], replicated
- enc_wv: bfloat16 [2, 1024, 1024], replicated
- enc_wo: bfloat16 [2, 16, 64, 1024], replicated
- enc_w1: bfloat16 [2, 1024, 2816], replicated
- enc_w2: bfloat16 [2, 2816, 1024], replicated
- dec_wq: bfloat16 [2, 1024, 1024], replicated
- dec_wk: bfloat16 [2, 1024, 1024], replicated
- dec_wv: bfloat16 [2, 1024, 1024], replicated
- dec_wo: bfloat16 [2, 16, 64, 1024], replicated
- crs_wq: bfloat16 [2, 1024, 1024], replicated
- crs_wk: bfloat16 [2, 1024, 1024], replicated
- crs_wv: bfloat16 [2, 1024, 1024], replicated
- crs_wo: bfloat16 [2, 16, 64, 1024], replicated
- dec_w1: bfloat16 [2, 1024, 2816], replicated
- dec_w2: bfloat16 [2, 2816, 1024], replicated
Outputs:
- output: bfloat16 [256, 96, 1024], P(('data', 'pair')), parts along dimension 0
There are 2 independent parts. The reference program is written for one: setup_inputs(seed, part) draws one part's arguments, and reference() takes and returns one part's arrays. A program takes and returns all parts, laid end to end along the dimension named above; an argument that names none is the same for every part.
All inputs are finite; a program needn't handle non-finite values.
Results may differ from the reference program's by a relative error of at most 0.0122378.
Values are sent between devices in bfloat16 or wider.
A program may use at most 1 GiB of HBM per device.

```python
import jax
import jax.numpy as jnp
from jax import lax

BATCH_ROWS = 128
SEQ_ENC = 256
SEQ_DEC = 96
D_MODEL = 1024
NUM_HEADS = 16
KV_HEADS = 16
HEAD_DIM = 64
FF_DIM = 2816
ENC_LAYERS = 2
DEC_LAYERS = 2


def setup_inputs(seed: int = 0, part: int = 0) -> dict:
    base_key = jax.random.key(seed)
    part_key = jax.random.fold_in(base_key, part)
    x_key, y_key = jax.random.split(part_key, 2)
    len_key = jax.random.fold_in(part_key, 3)
    weight_keys = jax.random.split(jax.random.key(seed + 1), 16)
    q_width = NUM_HEADS * HEAD_DIM
    kv_width = KV_HEADS * HEAD_DIM
    in_scale = D_MODEL ** -0.5
    out_scale = q_width ** -0.5
    attn_boost = SEQ_ENC ** 0.5 / 3.0

    def draw_normal(key, shape, scale):
        return (jax.random.normal(key, shape, jnp.float32) * scale).astype(jnp.bfloat16)

    enc_len = jax.random.randint(len_key, (BATCH_ROWS,), SEQ_ENC // 4, SEQ_ENC + 1, dtype=jnp.int32)
    enc_len = enc_len.at[0].set(SEQ_ENC).at[1].set(SEQ_ENC // 4)
    return {
        "x_enc": draw_normal(x_key, (BATCH_ROWS, SEQ_ENC, D_MODEL), 1.0),
        "enc_len": enc_len,
        "y_dec": draw_normal(y_key, (BATCH_ROWS, SEQ_DEC, D_MODEL), 1.0),
        "enc_wq": draw_normal(weight_keys[0], (ENC_LAYERS, D_MODEL, q_width), in_scale),
        "enc_wk": draw_normal(weight_keys[1], (ENC_LAYERS, D_MODEL, kv_width), in_scale),
        "enc_wv": draw_normal(weight_keys[2], (ENC_LAYERS, D_MODEL, kv_width), in_scale),
        "enc_wo": draw_normal(weight_keys[3], (ENC_LAYERS, NUM_HEADS, HEAD_DIM, D_MODEL), out_scale * attn_boost),
        "enc_w1": draw_normal(weight_keys[4], (ENC_LAYERS, D_MODEL, FF_DIM), in_scale),
        "enc_w2": draw_normal(weight_keys[5], (ENC_LAYERS, FF_DIM, D_MODEL), FF_DIM ** -0.5),
        "dec_wq": draw_normal(weight_keys[6], (DEC_LAYERS, D_MODEL, q_width), in_scale),
        "dec_wk": draw_normal(weight_keys[7], (DEC_LAYERS, D_MODEL, kv_width), in_scale),
        "dec_wv": draw_normal(weight_keys[8], (DEC_LAYERS, D_MODEL, kv_width), in_scale),
        "dec_wo": draw_normal(weight_keys[9], (DEC_LAYERS, NUM_HEADS, HEAD_DIM, D_MODEL), out_scale * 1.5),
        "crs_wq": draw_normal(weight_keys[10], (DEC_LAYERS, D_MODEL, q_width), in_scale),
        "crs_wk": draw_normal(weight_keys[11], (DEC_LAYERS, D_MODEL, kv_width), in_scale),
        "crs_wv": draw_normal(weight_keys[12], (DEC_LAYERS, D_MODEL, kv_width), in_scale),
        "crs_wo": draw_normal(weight_keys[13], (DEC_LAYERS, NUM_HEADS, HEAD_DIM, D_MODEL), out_scale * attn_boost),
        "dec_w1": draw_normal(weight_keys[14], (DEC_LAYERS, D_MODEL, FF_DIM), in_scale),
        "dec_w2": draw_normal(weight_keys[15], (DEC_LAYERS, FF_DIM, D_MODEL), FF_DIM ** -0.5),
    }


def rms_norm(hidden):
    x_wide = hidden.astype(jnp.float32)
    inv_rms = lax.rsqrt(jnp.mean(x_wide * x_wide, axis=-1, keepdims=True) + 1e-6)
    return (x_wide * inv_rms).astype(jnp.bfloat16)


def project(source, weight):
    return jnp.dot(source, weight, preferred_element_type=jnp.float32).astype(jnp.bfloat16)


def add_to(hidden, update):
    return (hidden.astype(jnp.float32) + update).astype(jnp.bfloat16)


def attend(query_rows, key_rows, value_rows, allowed, out_weight):
    q_len = query_rows.shape[0]
    k_len = key_rows.shape[0]
    q_heads = query_rows.reshape(q_len, KV_HEADS, NUM_HEADS // KV_HEADS, HEAD_DIM).astype(jnp.float32)
    k_heads = key_rows.reshape(k_len, KV_HEADS, HEAD_DIM).astype(jnp.float32)
    v_heads = value_rows.reshape(k_len, KV_HEADS, HEAD_DIM).astype(jnp.float32)
    scores = jnp.einsum("skrh,tkh->krst", q_heads, k_heads) * HEAD_DIM ** -0.5
    scores = jnp.where(allowed, scores, -1e30)
    attn_probs = jax.nn.softmax(scores, axis=-1).astype(jnp.bfloat16)
    context = jnp.einsum("krst,tkh->skrh", attn_probs.astype(jnp.float32), v_heads).astype(jnp.bfloat16)
    context = context.reshape(q_len, NUM_HEADS * HEAD_DIM)
    w_out = out_weight.reshape(NUM_HEADS * HEAD_DIM, D_MODEL)
    return jnp.dot(context, w_out, preferred_element_type=jnp.float32)


def feed_forward(hidden, w_up, w_down):
    normed = rms_norm(hidden)
    inner_act = jax.nn.gelu(jnp.dot(normed, w_up, preferred_element_type=jnp.float32)).astype(jnp.bfloat16)
    return add_to(hidden, jnp.dot(inner_act, w_down, preferred_element_type=jnp.float32))


def encode_row(x_row, length, enc_weights):
    allowed = jnp.arange(SEQ_ENC)[None, :] < length

    def layer_step(hidden, layer_weights):
        w_query, w_key, w_value, w_out, w_up, w_down = layer_weights
        normed = rms_norm(hidden)
        attn_out = attend(project(normed, w_query), project(normed, w_key), project(normed, w_value), allowed, w_out)
        return feed_forward(add_to(hidden, attn_out), w_up, w_down), None

    hidden, unused = lax.scan(layer_step, x_row, enc_weights)
    return rms_norm(hidden)


def decode_row(y_row, enc_row, length, dec_weights):
    cross_ok = jnp.arange(SEQ_ENC)[None, :] < length
    causal = jnp.arange(SEQ_DEC)[:, None] >= jnp.arange(SEQ_DEC)[None, :]

    def layer_step(hidden, layer_weights):
        w_query, w_key, w_value, w_out, c_query, c_key, c_value, c_out, w_up, w_down = layer_weights
        normed = rms_norm(hidden)
        self_out = attend(project(normed, w_query), project(normed, w_key), project(normed, w_value), causal, w_out)
        hidden = add_to(hidden, self_out)
        normed = rms_norm(hidden)
        cross_out = attend(project(normed, c_query), project(enc_row, c_key), project(enc_row, c_value), cross_ok, c_out)
        return feed_forward(add_to(hidden, cross_out), w_up, w_down), None

    hidden, unused = lax.scan(layer_step, y_row, dec_weights)
    return hidden


def reference(x_enc, enc_len, y_dec, enc_wq, enc_wk, enc_wv, enc_wo, enc_w1, enc_w2, dec_wq, dec_wk, dec_wv, dec_wo, crs_wq, crs_wk, crs_wv, crs_wo, dec_w1, dec_w2):
    enc_weights = (enc_wq, enc_wk, enc_wv, enc_wo, enc_w1, enc_w2)
    dec_weights = (dec_wq, dec_wk, dec_wv, dec_wo, crs_wq, crs_wk, crs_wv, crs_wo, dec_w1, dec_w2)
    enc_out = lax.map(lambda row_in: encode_row(row_in[0], row_in[1], enc_weights), (x_enc, enc_len))
    partner_out = jnp.roll(enc_out, BATCH_ROWS // 2, axis=0)
    partner_len = jnp.roll(enc_len, BATCH_ROWS // 2, axis=0)
    return lax.map(lambda row_in: decode_row(row_in[0], row_in[1], row_in[2], dec_weights), (y_dec, partner_out, partner_len))
```

```python
import functools

import jax
import jax.numpy as jnp
from jax import lax
from jax.experimental import pallas as pl
from jax.experimental.pallas import tpu as pltpu
from jax.sharding import PartitionSpec as P

BF16 = jnp.bfloat16
F32 = jnp.float32
I32 = jnp.int32

ROWS = 32
T_ENC = 256
T_DEC = 96
D = 1024
FF = 2816
PAIRS = 8
BIN = 512
NB = ROWS * T_ENC // BIN
CHUNKS = 4
CB = NB // CHUNKS
UNIT = 16
SCALE = 64 ** -0.5 * 1.4426950408889634
VMEM_MAX = 64 * 2**20 - 2**17

P_ORDER, P_OFF, P_LEN, P_GLOB, P_START, P_NBINS = 0, 32, 64, 96, 128, 160


def plan_kernel(len_ref, plan_ref, free, count, rbin, roff, rk):
    def clear(i, _):
        free[i] = BIN // UNIT
        count[i] = 0
        return 0

    lax.fori_loop(0, NB + 1, clear, 0)

    def by_size(i, nbins):
        size = T_ENC // UNIT - i

        def by_row(r, nbins):
            hit = (len_ref[r] + UNIT - 1) // UNIT == size

            @pl.when(hit)
            def _():
                b = lax.while_loop(lambda b: free[b] < size, lambda b: b + 1, jnp.int32(0))
                left = free[b]
                rbin[r] = b
                roff[r] = BIN - left * UNIT
                rk[r] = count[b]
                free[b] = left - size
                count[b] = count[b] + 1

            return nbins

        return lax.fori_loop(0, ROWS, by_row, nbins)

    lax.fori_loop(0, T_ENC // UNIT, by_size, 0)

    def starts(b, carry):
        total, nbins = carry
        plan_ref[P_START + b] = total
        c = count[b]
        return total + c, nbins + jnp.where(c > 0, 1, 0)

    total, nbins = lax.fori_loop(0, NB, starts, (jnp.int32(0), jnp.int32(0)))
    plan_ref[P_START + NB] = total

    def fill(i, _):
        plan_ref[i] = nbins
        return 0

    lax.fori_loop(P_START + NB + 1, 256, fill, 0)

    def place(r, _):
        b = rbin[r]
        pos = plan_ref[P_START + b] + rk[r]
        plan_ref[P_ORDER + pos] = r
        plan_ref[P_OFF + pos] = roff[r]
        plan_ref[P_LEN + pos] = len_ref[r]
        plan_ref[P_GLOB + pos] = b * BIN + roff[r]
        return 0

    lax.fori_loop(0, ROWS, place, 0)


def make_plan(enc_len):
    smem = pl.BlockSpec(memory_space=pltpu.SMEM)
    return pl.pallas_call(
        plan_kernel,
        out_shape=jax.ShapeDtypeStruct((256,), I32),
        in_specs=[smem],
        out_specs=smem,
        scratch_shapes=[pltpu.SMEM((32,), I32) for _ in range(5)],
        name="plan",
    )(enc_len)


def norm_rows(src, dst, rows, step=128):
    for m in range(0, rows, step):
        v = src[m:m + step, :].astype(F32)
        inv = lax.rsqrt(jnp.mean(v * v, axis=-1, keepdims=True) + 1e-6)
        dst[m:m + step, :] = (v * inv).astype(BF16)


def gelu(x):
    inner = x * (x * x * (0.044715 * 0.7978845608028654) + 0.7978845608028654)
    half = x * 0.5
    return half + half * jnp.tanh(inner)


def attend_pair(q, k, v, mask, vmask=None):
    tq, tk = q.shape[0], k.shape[0]
    lane = lax.broadcasted_iota(I32, (tq, 128), 1)
    low = (lane < 64)
    lowf = low.astype(F32).astype(BF16)
    q2 = jnp.concatenate([q * lowf, q * (1 - lowf)], axis=0)
    s = lax.dot_general(q2, k, (((1,), (1,)), ((), ())), preferred_element_type=F32)
    s = jnp.where(mask, s, -1e30)
    top = jnp.max(s, axis=-1, keepdims=True)
    e = jnp.exp2((s - top) * SCALE).astype(BF16)
    if vmask is not None:
        v = jnp.where(vmask, v, jnp.zeros_like(v))
    va = jnp.concatenate([v, jnp.ones_like(v)], axis=1)
    o = jnp.dot(e, va, preferred_element_type=F32)
    num = jnp.where(low, o[:tq, :128], o[tq:, :128])
    den = jnp.where(low, o[:tq, 128:], o[tq:, 128:])
    return (num / den).astype(BF16)


def enc_kernel(chunk, plan, x_hbm, wq_h, wk_h, wv_h, wo_h, w1_h, w2_h, out_ref,
               xb, n_s, q_s, k_s, v_s, c_s, inner, wq, wk, wv, wo, w1, w2, xsem, wsem):
    i = pl.program_id(0)
    b = chunk * CB + i
    nbins = plan[P_NBINS]
    slot = lax.rem(i, 2)
    weights = [(wq_h, wq), (wk_h, wk), (wv_h, wv), (wo_h, wo), (w1_h, w1), (w2_h, w2)]

    def weight_copy(j, l):
        return pltpu.make_async_copy(weights[j][0].at[l], weights[j][1].at[l], wsem.at[j, l])

    def row_copies(bb, sl, start):
        def per_row(pos, _):
            row, off = plan[P_ORDER + pos], plan[P_OFF + pos]
            units = (plan[P_LEN + pos] + UNIT - 1) // UNIT
            for bit in (16, 8, 4, 2, 1):
                @pl.when((units & bit) != 0)
                def _():
                    at = (units & ~(2 * bit - 1)) * UNIT
                    cp = pltpu.make_async_copy(
                        x_hbm.at[row, pl.ds(pl.multiple_of(at, UNIT), bit * UNIT), :],
                        xb.at[sl, pl.ds(pl.multiple_of(off + at, UNIT), bit * UNIT), :],
                        xsem.at[sl])
                    if start:
                        cp.start()
                    else:
                        cp.wait()
            return 0

        lax.fori_loop(plan[P_START + bb], plan[P_START + bb + 1], per_row, 0)

    @pl.when(jnp.logical_and(i == 0, b < nbins))
    def _():
        row_copies(b, slot, True)
        for l in range(2):
            for j in range(6):
                weight_copy(j, l).start()
        tail = slice(BIN, BIN + T_ENC)
        for ref in (q_s, k_s, v_s):
            ref[tail, :] = jnp.zeros((T_ENC, D), BF16)
        c_s[...] = jnp.zeros_like(c_s)

    @pl.when(jnp.logical_and(i + 1 < CB, b + 1 < nbins))
    def _():
        row_copies(b + 1, 1 - slot, True)

    @pl.when(b >= nbins)
    def _():
        out_ref[...] = jnp.zeros_like(out_ref)

    @pl.when(b < nbins)
    def _():
        row_copies(b, slot, False)
        first, last = plan[P_START + b], plan[P_START + b + 1]
        used = plan[P_OFF + last - 1] + (plan[P_LEN + last - 1] + UNIT - 1) // UNIT * UNIT
        h = xb.at[slot]

        def zero_unit(u, _):
            h[pl.ds(pl.multiple_of(u * UNIT, UNIT), UNIT), :] = jnp.zeros((UNIT, D), BF16)
            return 0

        lax.fori_loop(used // UNIT, BIN // UNIT, zero_unit, 0)

        def need(j, l):
            @pl.when(i == 0)
            def _():
                weight_copy(j, l).wait()

        def layer(l, _):
            for j in range(3):
                need(j, l)
            norm_rows(h, n_s, BIN)
            for w, dst in ((wq, q_s), (wk, k_s), (wv, v_s)):
                for n in range(0, D, 256):
                    dst[0:BIN, n:n + 256] = jnp.dot(n_s[...], w[l, :, n:n + 256], preferred_element_type=F32).astype(BF16)

            def per_row(pos, _):
                off = pl.multiple_of(plan[P_OFF + pos], UNIT)
                length = plan[P_LEN + pos]

                def run(t):
                    mask = lax.broadcasted_iota(I32, (2 * t, t), 1) < length
                    rows = pl.ds(off, t)

                    def pair(p, _):
                        cols = pl.ds(pl.multiple_of(p * 128, 128), 128)
                        c_s[rows, cols] = attend_pair(q_s[rows, cols], k_s[rows, cols], v_s[rows, cols], mask)
                        return 0

                    lax.fori_loop(0, PAIRS, pair, 0, unroll=2)

                for lo, t in ((0, 128), (128, 192), (192, 256)):
                    @pl.when(jnp.logical_and(length > lo, length <= t))
                    def _():
                        run(t)

                return 0

            lax.fori_loop(first, last, per_row, 0)
            need(3, l)
            need(4, l)
            for n in range(0, D, 256):
                u = jnp.dot(c_s[0:BIN, :], wo[l, :, n:n + 256], preferred_element_type=F32)
                h[:, n:n + 256] = (h[:, n:n + 256].astype(F32) + u).astype(BF16)
            norm_rows(h, n_s, BIN)
            for n in range(0, FF, 256):
                u = jnp.dot(n_s[...], w1[l, :, n:n + 256], preferred_element_type=F32)
                inner[:, n:n + 256] = gelu(u).astype(BF16)
            need(5, l)
            for n in range(0, D, 256):
                u = jnp.dot(inner[...], w2[l, :, n:n + 256], preferred_element_type=F32)
                h[:, n:n + 256] = (h[:, n:n + 256].astype(F32) + u).astype(BF16)
            return 0

        lax.fori_loop(0, 2, layer, 0)
        norm_rows(h, out_ref, BIN)


def encode_chunk(chunk, plan, x_enc, weights):
    hbm = pl.BlockSpec(memory_space=pl.ANY)
    vm = lambda *s: pltpu.VMEM(s, BF16)
    tokens = BIN + T_ENC
    return pl.pallas_call(
        functools.partial(enc_kernel, chunk),
        out_shape=jax.ShapeDtypeStruct((CB * BIN, D), BF16),
        grid_spec=pltpu.PrefetchScalarGridSpec(
            num_scalar_prefetch=1,
            grid=(CB,),
            in_specs=[hbm] * 7,
            out_specs=pl.BlockSpec((BIN, D), lambda i, plan: (i, 0)),
            scratch_shapes=[
                vm(2, BIN, D), vm(BIN, D), vm(tokens, D), vm(tokens, D), vm(tokens, D), vm(tokens, D), vm(BIN, FF),
                vm(2, D, D), vm(2, D, D), vm(2, D, D), vm(2, D, D), vm(2, D, FF), vm(2, FF, D),
                pltpu.SemaphoreType.DMA((2,)), pltpu.SemaphoreType.DMA((6, 2)),
            ],
        ),
        compiler_params=pltpu.CompilerParams(vmem_limit_bytes=VMEM_MAX, dimension_semantics=("arbitrary",)),
        cost_estimate=pl.CostEstimate(flops=80_000_000_000, bytes_accessed=60_000_000, transcendentals=0),
        name="encode",
    )(plan, x_enc, *weights)


def cross_kernel(base, plan, h_ref, wk_ref, wv_ref, k0_ref, v0_ref, k1_ref, v1_ref):
    @pl.when(base + pl.program_id(0) < plan[P_NBINS])
    def _():
        for l, k_ref, v_ref in ((0, k0_ref, v0_ref), (1, k1_ref, v1_ref)):
            for w, dst in ((wk_ref, k_ref), (wv_ref, v_ref)):
                for n in range(0, D, 256):
                    dst[:, n:n + 256] = jnp.dot(h_ref[...], w[l, :, n:n + 256], preferred_element_type=F32).astype(BF16)


def cross_keys(base, plan, h, wk, wv):
    tokens = h.shape[0]
    whole = pl.BlockSpec((2, D, D), lambda i, plan: (0, 0, 0))

    def block(i, plan):
        return jnp.minimum(i, jnp.maximum(plan[P_NBINS] - 1 - base, 0)), 0

    spec = pl.BlockSpec((BIN, D), block)
    return pl.pallas_call(
        functools.partial(cross_kernel, base),
        out_shape=[jax.ShapeDtypeStruct((tokens, D), BF16)] * 4,
        grid_spec=pltpu.PrefetchScalarGridSpec(
            num_scalar_prefetch=1, grid=(tokens // BIN,), in_specs=[spec, whole, whole], out_specs=[spec] * 4),
        compiler_params=pltpu.CompilerParams(vmem_limit_bytes=VMEM_MAX, dimension_semantics=("arbitrary",)),
        cost_estimate=pl.CostEstimate(flops=8 * tokens * D * D, bytes_accessed=10 * tokens * D, transcendentals=0),
        name="cross_keys",
    )(plan, h, wk, wv)


G = 4
MG = G * T_DEC
HALF = ROWS // 2
HALF_TOKENS = NB * BIN // 2


def dec_kernel(half, plan, *refs):
    nkv = half + 1
    y_hbm = refs[0]
    kv_hbm = refs[1:1 + 4 * nkv]
    w_hbm = refs[1 + 4 * nkv:9 + 4 * nkv]
    rest = refs[9 + 4 * nkv + (1 if half else 0):]
    out_hbm, zb, n_s, q_s, k_s, v_s, c_s, inner, kb, vb = rest[:10]
    w_s = rest[10:18]
    ysem, osem, kvsem, wsem = rest[18:]
    wq, wk, wv, wo, cq, co, w1, w2 = w_s
    i = pl.program_id(0)
    groups = pl.num_programs(0)
    slot = lax.rem(i, 2)

    def weight_copy(j, l):
        return pltpu.make_async_copy(w_hbm[j].at[l], w_s[j].at[l], wsem.at[j, l])

    def first_row(g):
        return half * HALF + g * G

    def y_copy(g, sl, r):
        row = plan[P_ORDER + first_row(g) + r]
        return pltpu.make_async_copy(y_hbm.at[row], zb.at[sl, pl.ds(r * T_DEC, T_DEC), :], ysem.at[sl])

    def out_copy(g, sl, r):
        row = plan[P_ORDER + first_row(g) + r]
        return pltpu.make_async_copy(zb.at[sl, pl.ds(r * T_DEC, T_DEC), :], out_hbm.at[row], osem.at[sl])

    def kv_copies(l, start):
        def per_row(r, _):
            pos = first_row(i) + r
            at_glob = plan[P_GLOB + pos]
            units = (plan[P_LEN + pos] + UNIT - 1) // UNIT
            for part in range(nkv):
                for which, dst in ((0, kb), (1, vb)):
                    src = (kv_hbm[4 * part + which], kv_hbm[4 * part + 2 + which])

                    for bit in (16, 8, 4, 2, 1):
                        inside = jnp.logical_and(at_glob >= part * HALF_TOKENS, at_glob < (part + 1) * HALF_TOKENS)

                        @pl.when(jnp.logical_and(inside, (units & bit) != 0))
                        def _():
                            at = (units & ~(2 * bit - 1)) * UNIT
                            cp = pltpu.make_async_copy(
                                src[l].at[pl.ds(pl.multiple_of(at_glob - part * HALF_TOKENS + at, UNIT), bit * UNIT), :],
                                dst.at[r, pl.ds(pl.multiple_of(at, UNIT), bit * UNIT), :],
                                kvsem)
                            if start:
                                cp.start()
                            else:
                                cp.wait()
            return 0

        lax.fori_loop(0, G, per_row, 0)

    @pl.when(i == 0)
    def _():
        for r in range(G):
            y_copy(0, 0, r).start()
        for l in range(2):
            for j in range(8):
                weight_copy(j, l).start()

    @pl.when(i >= 1)
    def _():
        for r in range(G):
            out_copy(i - 1, 1 - slot, r).wait()

    @pl.when(i + 1 < groups)
    def _():
        for r in range(G):
            y_copy(i + 1, 1 - slot, r).start()

    for r in range(G):
        y_copy(i, slot, r).wait()
    z = zb.at[slot]

    def need(j, l):
        @pl.when(i == 0)
        def _():
            weight_copy(j, l).wait()

    def add_to_z(src, w, l):
        for n in range(0, D, 256):
            u = jnp.dot(src[...], w[l, :, n:n + 256], preferred_element_type=F32)
            z[:, n:n + 256] = (z[:, n:n + 256].astype(F32) + u).astype(BF16)

    for l in range(2):
        kv_copies(l, True)
        for j in range(3):
            need(j, l)
        norm_rows(z, n_s, MG)
        for w, dst in ((wq, q_s), (wk, k_s), (wv, v_s)):
            for n in range(0, D, 256):
                dst[:, n:n + 256] = jnp.dot(n_s[...], w[l, :, n:n + 256], preferred_element_type=F32).astype(BF16)
        row_at = lax.broadcasted_iota(I32, (2 * T_DEC, T_DEC), 0)
        row_at = jnp.where(row_at >= T_DEC, row_at - T_DEC, row_at)
        causal = row_at >= lax.broadcasted_iota(I32, (2 * T_DEC, T_DEC), 1)

        def self_pair(p, _):
            cols = pl.ds(pl.multiple_of(p * 128, 128), 128)
            for r in range(G):
                rows = slice(r * T_DEC, (r + 1) * T_DEC)
                c_s[rows, cols] = attend_pair(q_s[rows, cols], k_s[rows, cols], v_s[rows, cols], causal)
            return 0

        lax.fori_loop(0, PAIRS, self_pair, 0)
        need(3, l)
        need(4, l)
        add_to_z(c_s, wo, l)
        norm_rows(z, n_s, MG)
        for n in range(0, D, 256):
            q_s[:, n:n + 256] = jnp.dot(n_s[...], cq[l, :, n:n + 256], preferred_element_type=F32).astype(BF16)
        kv_copies(l, False)

        def cross_pair(p, _):
            cols = pl.ds(pl.multiple_of(p * 128, 128), 128)
            for r in range(G):
                length = plan[P_LEN + first_row(i) + r]
                mask = lax.broadcasted_iota(I32, (2 * T_DEC, T_ENC), 1) < length
                vmask = lax.broadcasted_iota(I32, (T_ENC, 128), 0) < length
                rows = slice(r * T_DEC, (r + 1) * T_DEC)
                c_s[rows, cols] = attend_pair(q_s[rows, cols], kb[r, :, cols], vb[r, :, cols], mask, vmask)
            return 0

        lax.fori_loop(0, PAIRS, cross_pair, 0)
        need(5, l)
        need(6, l)
        add_to_z(c_s, co, l)
        norm_rows(z, n_s, MG)
        for n in range(0, FF, 256):
            u = jnp.dot(n_s[...], w1[l, :, n:n + 256], preferred_element_type=F32)
            inner[:, n:n + 256] = gelu(u).astype(BF16)
        need(7, l)
        add_to_z(inner, w2, l)

    for r in range(G):
        out_copy(i, slot, r).start()

    @pl.when(i == groups - 1)
    def _():
        for r in range(G):
            out_copy(i, slot, r).wait()


def decode_half(half, plan, y_dec, kvs, weights, prev):
    hbm = pl.BlockSpec(memory_space=pl.ANY)
    vm = lambda *s: pltpu.VMEM(s, BF16)
    ins = [y_dec, *kvs, *weights] + ([prev] if half else [])
    return pl.pallas_call(
        functools.partial(dec_kernel, half),
        out_shape=jax.ShapeDtypeStruct((ROWS, T_DEC, D), BF16),
        grid_spec=pltpu.PrefetchScalarGridSpec(
            num_scalar_prefetch=1,
            grid=(HALF // G,),
            in_specs=[hbm] * len(ins),
            out_specs=hbm,
            scratch_shapes=[
                vm(2, MG, D), vm(MG, D), vm(MG, D), vm(MG, D), vm(MG, D), vm(MG, D), vm(MG, FF),
                vm(G, T_ENC, D), vm(G, T_ENC, D),
                vm(2, D, D), vm(2, D, D), vm(2, D, D), vm(2, D, D), vm(2, D, D), vm(2, D, D), vm(2, D, FF), vm(2, FF, D),
                pltpu.SemaphoreType.DMA((2,)), pltpu.SemaphoreType.DMA((2,)), pltpu.SemaphoreType.DMA,
                pltpu.SemaphoreType.DMA((8, 2)),
            ],
        ),
        input_output_aliases={len(ins): 0} if half else {},
        compiler_params=pltpu.CompilerParams(vmem_limit_bytes=VMEM_MAX, dimension_semantics=("arbitrary",)),
        cost_estimate=pl.CostEstimate(flops=90_000_000_000, bytes_accessed=100_000_000, transcendentals=0),
        name="decode",
    )(plan, *ins)


def solution(mesh):
    pair_size = mesh.shape["pair"]
    to_partner = [(source, (source + pair_size // 2) % pair_size) for source in range(pair_size)]
    row_spec = P(("data", "pair"))
    full_spec = P()

    def per_device(x_enc, enc_len, y_dec, enc_wq, enc_wk, enc_wv, enc_wo, enc_w1, enc_w2, dec_wq, dec_wk, dec_wv, dec_wo, crs_wq, crs_wk, crs_wv, crs_wo, dec_w1, dec_w2):
        flat = lambda w: w.reshape(2, D, D)
        plan = make_plan(enc_len)
        partner_plan = lax.ppermute(plan, "pair", to_partner)
        enc_weights = (enc_wq, enc_wk, enc_wv, flat(enc_wo), enc_w1, enc_w2)
        enc_out = []
        for chunk in range(CHUNKS):
            h = encode_chunk(chunk, plan, x_enc, enc_weights)
            enc_out.append(lax.ppermute(h, "pair", to_partner))
        dec_weights = (dec_wq, dec_wk, dec_wv, flat(dec_wo), crs_wq, flat(crs_wo), dec_w1, dec_w2)
        out, kvs = None, []
        for half in range(2):
            h = jnp.concatenate(enc_out[2 * half:2 * half + 2], axis=0)
            kvs += cross_keys(half * NB // 2, partner_plan, h, crs_wk, crs_wv)
            out = decode_half(half, partner_plan, y_dec, kvs, dec_weights, out)
        return out

    return jax.shard_map(per_device, mesh=mesh, in_specs=(row_spec, row_spec, row_spec) + (full_spec,) * 16, out_specs=row_spec, check_vma=False)
```

```python
import functools

import jax
import jax.numpy as jnp
from jax import lax
from jax.experimental import pallas as pl
from jax.experimental.pallas import tpu as pltpu
from jax.sharding import PartitionSpec as P

BF16 = jnp.bfloat16
F32 = jnp.float32
I32 = jnp.int32

ROWS = 32
T_ENC = 256
T_DEC = 96
D = 1024
FF = 2816
PAIRS = 8
BIN = 512
NB = ROWS * T_ENC // BIN
CHUNKS = (4, 4, 2, 2, 4)
TN = 256
TF = 256
NS = 128
UNIT = 16
SCALE = 64 ** -0.5 * 1.4426950408889634
VMEM_MAX = 64 * 2**20 - 2**17

P_ORDER, P_OFF, P_LEN, P_GLOB, P_START, P_NBINS = 0, 32, 64, 96, 128, 160


def plan_kernel(len_ref, rank_ref, plan_ref, free, count, rbin, roff, rk, order):
    def clear(i, _):
        free[i] = BIN // UNIT
        count[i] = 0
        order[rank_ref[i]] = i
        order[rank_ref[i + NB]] = i + NB
        return 0

    lax.fori_loop(0, NB, clear, 0, unroll=4)

    def by_rank(i, _):
        r = order[i]
        size = (len_ref[r] + UNIT - 1) // UNIT
        b = lax.while_loop(lambda b: free[b] < size, lambda b: b + 1, jnp.int32(0))
        left = free[b]
        rbin[r] = b
        roff[r] = BIN - left * UNIT
        rk[r] = count[b]
        free[b] = left - size
        count[b] = count[b] + 1
        return 0

    lax.fori_loop(0, ROWS, by_rank, 0)

    def starts(b, carry):
        total, nbins = carry
        plan_ref[P_START + b] = total
        c = count[b]
        return total + c, nbins + jnp.where(c > 0, 1, 0)

    total, nbins = lax.fori_loop(0, NB, starts, (jnp.int32(0), jnp.int32(0)))
    plan_ref[P_START + NB] = total

    plan_ref[P_NBINS] = nbins

    def place(r, _):
        b = rbin[r]
        pos = plan_ref[P_START + b] + rk[r]
        plan_ref[P_ORDER + pos] = r
        plan_ref[P_OFF + pos] = roff[r]
        plan_ref[P_LEN + pos] = len_ref[r]
        plan_ref[P_GLOB + pos] = b * BIN + roff[r]
        return 0

    lax.fori_loop(0, ROWS, place, 0, unroll=4)


def make_plan(enc_len):
    units = (enc_len + UNIT - 1) // UNIT
    at = jnp.arange(ROWS)
    before = (units[None, :] > units[:, None]) | ((units[None, :] == units[:, None]) & (at[None, :] < at[:, None]))
    rank = jnp.sum(before.astype(I32), axis=1)
    smem = pl.BlockSpec(memory_space=pltpu.SMEM)
    return pl.pallas_call(
        plan_kernel,
        out_shape=jax.ShapeDtypeStruct((256,), I32),
        in_specs=[smem, smem],
        out_specs=smem,
        scratch_shapes=[pltpu.SMEM((32,), I32) for _ in range(6)],
        name="plan",
    )(enc_len, rank)


def norm_rows(src, dst, rows):
    step = NS
    for m in range(0, rows, step):
        v = src[m:m + step, :].astype(F32)
        inv = lax.rsqrt(jnp.mean(v * v, axis=-1, keepdims=True) + 1e-6)
        dst[m:m + step, :] = (v * inv).astype(BF16)


def gelu(x):
    inner = x * (x * x * (0.044715 * 0.7978845608028654) + 0.7978845608028654)
    half = x * 0.5
    return half + half * jnp.tanh(inner)


def attend_pair(q, k, v, mask, vmask=None):
    tq, tk = q.shape[0], k.shape[0]
    lane = lax.broadcasted_iota(I32, (tq, 128), 1)
    low = (lane < 64)
    lowf = low.astype(F32).astype(BF16)
    q2 = jnp.concatenate([q * lowf, q * (1 - lowf)], axis=0)
    s = lax.dot_general(q2, k, (((1,), (1,)), ((), ())), preferred_element_type=F32)
    s = jnp.where(mask, s, -1e30)
    top = jnp.max(s, axis=-1, keepdims=True)
    e = jnp.exp2((s - top) * SCALE).astype(BF16)
    if vmask is not None:
        v = jnp.where(vmask, v, jnp.zeros_like(v))
    va = jnp.concatenate([v, jnp.ones_like(v)], axis=1)
    o = jnp.dot(e, va, preferred_element_type=F32)
    num = jnp.where(low, o[:tq, :128], o[tq:, :128])
    den = jnp.where(low, o[:tq, 128:], o[tq:, 128:])
    return (num / den).astype(BF16)


def enc_kernel(base, plan, x_hbm, wq_h, wk_h, wv_h, wo_h, w1_h, w2_h, after, out_ref,
               xb, n_s, q_s, k_s, v_s, c_s, inner, wq, wk, wv, wo, w1, w2, xsem, wsem):
    i = pl.program_id(0)
    b = base + i
    nbins = plan[P_NBINS]
    slot = lax.rem(i, 2)
    weights = [(wq_h, wq), (wk_h, wk), (wv_h, wv), (wo_h, wo), (w1_h, w1), (w2_h, w2)]

    def weight_copy(j, l):
        return pltpu.make_async_copy(weights[j][0].at[l], weights[j][1].at[l], wsem.at[j, l])

    def row_copies(bb, sl, start):
        def per_row(pos, _):
            row, off = plan[P_ORDER + pos], plan[P_OFF + pos]
            units = (plan[P_LEN + pos] + UNIT - 1) // UNIT
            for bit in (16, 8, 4, 2, 1):
                @pl.when((units & bit) != 0)
                def _():
                    at = (units & ~(2 * bit - 1)) * UNIT
                    cp = pltpu.make_async_copy(
                        x_hbm.at[row, pl.ds(pl.multiple_of(at, UNIT), bit * UNIT), :],
                        xb.at[sl, pl.ds(pl.multiple_of(off + at, UNIT), bit * UNIT), :],
                        xsem.at[sl])
                    if start:
                        cp.start()
                    else:
                        cp.wait()
            return 0

        lax.fori_loop(plan[P_START + bb], plan[P_START + bb + 1], per_row, 0)

    @pl.when(jnp.logical_and(i == 0, b < nbins))
    def _():
        row_copies(b, slot, True)
        for l in range(2):
            for j in range(6):
                weight_copy(j, l).start()
        tail = slice(BIN, BIN + T_ENC)
        for ref in (q_s, k_s, v_s):
            ref[tail, :] = jnp.zeros((T_ENC, D), BF16)
        c_s[...] = jnp.zeros_like(c_s)

    @pl.when(jnp.logical_and(i + 1 < pl.num_programs(0), b + 1 < nbins))
    def _():
        row_copies(b + 1, 1 - slot, True)

    @pl.when(b >= nbins)
    def _():
        out_ref[...] = jnp.zeros_like(out_ref)

    @pl.when(b < nbins)
    def _():
        row_copies(b, slot, False)
        first, last = plan[P_START + b], plan[P_START + b + 1]
        used = plan[P_OFF + last - 1] + (plan[P_LEN + last - 1] + UNIT - 1) // UNIT * UNIT
        h = xb.at[slot]

        def zero_unit(u, _):
            h[pl.ds(pl.multiple_of(u * UNIT, UNIT), UNIT), :] = jnp.zeros((UNIT, D), BF16)
            return 0

        lax.fori_loop(used // UNIT, BIN // UNIT, zero_unit, 0)

        def need(j, l):
            @pl.when(i == 0)
            def _():
                weight_copy(j, l).wait()

        def layer(l, _):
            for j in range(3):
                need(j, l)
            norm_rows(h, n_s, BIN)
            for w, dst in ((wq, q_s), (wk, k_s), (wv, v_s)):
                for n in range(0, D, TN):
                    dst[0:BIN, n:n + TN] = jnp.dot(n_s[...], w[l, :, n:n + TN], preferred_element_type=F32).astype(BF16)

            def per_row(pos, _):
                off = pl.multiple_of(plan[P_OFF + pos], UNIT)
                length = plan[P_LEN + pos]

                def run(t):
                    mask = lax.broadcasted_iota(I32, (2 * t, T_ENC), 1) < length
                    for p in range(PAIRS):
                        cols = slice(p * 128, (p + 1) * 128)
                        c_s[pl.ds(off, t), cols] = attend_pair(
                            q_s[pl.ds(off, t), cols], k_s[pl.ds(off, T_ENC), cols], v_s[pl.ds(off, T_ENC), cols], mask)

                for t in range(96, T_ENC + 1, 32):
                    lo = 0 if t == 96 else t - 32

                    @pl.when(jnp.logical_and(length > lo, length <= t))
                    def _():
                        run(t)

                return 0

            lax.fori_loop(first, last, per_row, 0)
            for j in range(3, 6):
                need(j, l)
            for n in range(0, D, TN):
                u = jnp.dot(c_s[0:BIN, :], wo[l, :, n:n + TN], preferred_element_type=F32)
                h[:, n:n + TN] = (h[:, n:n + TN].astype(F32) + u).astype(BF16)
            norm_rows(h, n_s, BIN)
            for n in range(0, FF, TF):
                u = jnp.dot(n_s[...], w1[l, :, n:n + TF], preferred_element_type=F32)
                inner[:, n:n + TF] = gelu(u).astype(BF16)
            for n in range(0, D, TN):
                u = jnp.dot(inner[...], w2[l, :, n:n + TN], preferred_element_type=F32)
                h[:, n:n + TN] = (h[:, n:n + TN].astype(F32) + u).astype(BF16)
            return 0

        lax.fori_loop(0, 2, layer, 0)
        norm_rows(h, out_ref, BIN)


def encode_chunk(base, bins, plan, x_enc, weights, after):
    hbm = pl.BlockSpec(memory_space=pl.ANY)
    vm = lambda *s: pltpu.VMEM(s, BF16)
    tokens = BIN + T_ENC
    return pl.pallas_call(
        functools.partial(enc_kernel, base),
        out_shape=jax.ShapeDtypeStruct((bins * BIN, D), BF16),
        grid_spec=pltpu.PrefetchScalarGridSpec(
            num_scalar_prefetch=1,
            grid=(bins,),
            in_specs=[hbm] * 8,
            out_specs=pl.BlockSpec((BIN, D), lambda i, plan: (i, 0)),
            scratch_shapes=[
                vm(2, BIN, D), vm(BIN, D), vm(tokens, D), vm(tokens, D), vm(tokens, D), vm(tokens, D), vm(BIN, FF),
                vm(2, D, D), vm(2, D, D), vm(2, D, D), vm(2, D, D), vm(2, D, FF), vm(2, FF, D),
                pltpu.SemaphoreType.DMA((2,)), pltpu.SemaphoreType.DMA((6, 2)),
            ],
        ),
        compiler_params=pltpu.CompilerParams(vmem_limit_bytes=VMEM_MAX, dimension_semantics=("arbitrary",)),
        cost_estimate=pl.CostEstimate(flops=20_000_000_000 * bins, bytes_accessed=60_000_000, transcendentals=0),
        name="encode",
    )(plan, x_enc, *weights, after)


def cross_kernel(base, sizes, plan, *refs):
    h_hbm = refs[:len(sizes)]
    wk_ref, wv_ref, after, k_ref, v_ref, hb, hsem = refs[len(sizes):]
    i = pl.program_id(0)
    slot = lax.rem(i, 2)
    nbins = plan[P_NBINS] - base

    def fetch(at, sl, start):
        lo = 0
        for ref, size in zip(h_hbm, sizes):
            @pl.when(jnp.logical_and(at < nbins, jnp.logical_and(at >= lo, at < lo + size)))
            def _(ref=ref, lo=lo):
                cp = pltpu.make_async_copy(
                    ref.at[pl.ds(pl.multiple_of((at - lo) * BIN, BIN), BIN), :], hb.at[sl], hsem.at[sl])
                if start:
                    cp.start()
                else:
                    cp.wait()
            lo += size

    @pl.when(i == 0)
    def _():
        fetch(i, slot, True)

    @pl.when(i + 1 < sum(sizes))
    def _():
        fetch(i + 1, 1 - slot, True)

    fetch(i, slot, False)

    @pl.when(i < nbins)
    def _():
        for l in range(2):
            for w, dst in ((wk_ref, k_ref), (wv_ref, v_ref)):
                for n in range(0, D, TN):
                    dst[l, :, n:n + TN] = jnp.dot(hb[slot], w[l, :, n:n + TN], preferred_element_type=F32).astype(BF16)


def cross_keys(base, plan, hs, wk, wv, after):
    sizes = tuple(h.shape[0] // BIN for h in hs)
    tokens = sum(sizes) * BIN
    hbm = pl.BlockSpec(memory_space=pl.ANY)
    whole = pl.BlockSpec((2, D, D), lambda i, plan: (0, 0, 0))

    def block(i, plan):
        return 0, jnp.minimum(i, jnp.maximum(plan[P_NBINS] - 1 - base, 0)), 0

    spec = pl.BlockSpec((2, BIN, D), block)
    return pl.pallas_call(
        functools.partial(cross_kernel, base, sizes),
        out_shape=[jax.ShapeDtypeStruct((2, tokens + BIN, D), BF16)] * 2,
        grid_spec=pltpu.PrefetchScalarGridSpec(
            num_scalar_prefetch=1, grid=(sum(sizes),), in_specs=[hbm] * len(hs) + [whole, whole, hbm], out_specs=[spec] * 2,
            scratch_shapes=[pltpu.VMEM((2, BIN, D), BF16), pltpu.SemaphoreType.DMA((2,))]),
        compiler_params=pltpu.CompilerParams(vmem_limit_bytes=VMEM_MAX, dimension_semantics=("arbitrary",)),
        cost_estimate=pl.CostEstimate(flops=8 * tokens * D * D, bytes_accessed=10 * tokens * D, transcendentals=0),
        name="cross_keys",
    )(plan, *hs, wk, wv, after)


G = 8
MG = G * T_DEC
HALF = ROWS // 2
HALF_TOKENS = NB * BIN // 2


def dec_kernel(half, plan, *refs):
    nkv = half + 1
    y_hbm = refs[0]
    kv_hbm = refs[1:1 + 2 * nkv]
    w_hbm = refs[1 + 2 * nkv:9 + 2 * nkv]
    rest = refs[9 + 2 * nkv + (1 if half else 0):]
    out_hbm, zb, n_s, qkv, c_s, kb, vb = rest[:7]
    w_s = rest[7:15]
    ysem, osem, kvsem, wsem = rest[15:]
    inner = qkv.at[0:MG, 0:FF]
    wq, wk, wv, wo, cq, co, w1, w2 = w_s
    i = pl.program_id(0)
    groups = pl.num_programs(0)
    slot = lax.rem(i, 2)

    def weight_copy(j, l):
        return pltpu.make_async_copy(w_hbm[j].at[l], w_s[j].at[l], wsem.at[j, l])

    def first_row(g):
        return half * HALF + g * G

    def y_copy(g, sl, r):
        row = plan[P_ORDER + first_row(g) + r]
        return pltpu.make_async_copy(y_hbm.at[row], zb.at[sl, pl.ds(r * T_DEC, T_DEC), :], ysem.at[sl])

    def out_copy(g, sl, r):
        row = plan[P_ORDER + first_row(g) + r]
        return pltpu.make_async_copy(zb.at[sl, pl.ds(r * T_DEC, T_DEC), :], out_hbm.at[row], osem.at[sl])

    def kv_start(l, r):
        at = plan[P_GLOB + first_row(i) + r]
        sl = lax.rem(r, 2)
        for part in range(nkv):
            @pl.when(jnp.logical_and(at >= part * HALF_TOKENS, at < (part + 1) * HALF_TOKENS))
            def _():
                rows = pl.ds(pl.multiple_of(at - part * HALF_TOKENS, UNIT), T_ENC)
                pltpu.make_async_copy(kv_hbm[2 * part].at[l, rows, :], kb.at[sl], kvsem.at[0, sl]).start()
                pltpu.make_async_copy(kv_hbm[2 * part + 1].at[l, rows, :], vb.at[sl], kvsem.at[1, sl]).start()

    def kv_wait(l, r):
        sl = lax.rem(r, 2)
        pltpu.make_async_copy(kv_hbm[0].at[l, pl.ds(0, T_ENC), :], kb.at[sl], kvsem.at[0, sl]).wait()
        pltpu.make_async_copy(kv_hbm[1].at[l, pl.ds(0, T_ENC), :], vb.at[sl], kvsem.at[1, sl]).wait()

    @pl.when(i == 0)
    def _():
        qkv[MG:MG + 64, :] = jnp.zeros((64, 3 * D), BF16)
        for r in range(G):
            y_copy(0, 0, r).start()
        for l in range(2):
            for j in range(8):
                weight_copy(j, l).start()

    @pl.when(i >= 1)
    def _():
        for r in range(G):
            out_copy(i - 1, 1 - slot, r).wait()

    @pl.when(i + 1 < groups)
    def _():
        for r in range(G):
            y_copy(i + 1, 1 - slot, r).start()

    for r in range(G):
        y_copy(i, slot, r).wait()
    z = zb.at[slot]

    def need(j, l):
        @pl.when(i == 0)
        def _():
            weight_copy(j, l).wait()

    def add_to_z(src, w, l):
        for n in range(0, D, TN):
            u = jnp.dot(src[...], w[l, :, n:n + TN], preferred_element_type=F32)
            z[:, n:n + TN] = (z[:, n:n + TN].astype(F32) + u).astype(BF16)

    def layer(l, _):
        kv_start(l, jnp.int32(0))
        kv_start(l, jnp.int32(1))
        for j in range(3):
            need(j, l)
        norm_rows(z, n_s, MG)
        for j, w in enumerate((wq, wk, wv)):
            for n in range(0, D, TN):
                qkv[0:MG, j * D + n:j * D + n + TN] = jnp.dot(n_s[...], w[l, :, n:n + TN], preferred_element_type=F32).astype(BF16)
        two = 2 * T_DEC
        row_at = lax.broadcasted_iota(I32, (2 * two, T_ENC), 0)
        row_at = jnp.where(row_at >= two, row_at - two, row_at)
        col_at = lax.broadcasted_iota(I32, (2 * two, T_ENC), 1)
        causal = (row_at >= col_at) & ((row_at < T_DEC) | (col_at >= T_DEC))

        def self_rows(r, _):
            at = pl.multiple_of(r * two, 64)
            for p in range(PAIRS):
                cols = slice(p * 128, (p + 1) * 128)
                c_s[pl.ds(at, two), cols] = attend_pair(
                    qkv[pl.ds(at, two), p * 128:(p + 1) * 128],
                    qkv[pl.ds(at, T_ENC), D + p * 128:D + (p + 1) * 128],
                    qkv[pl.ds(at, T_ENC), 2 * D + p * 128:2 * D + (p + 1) * 128], causal)
            return 0

        lax.fori_loop(0, G // 2, self_rows, 0)
        need(3, l)
        need(4, l)
        add_to_z(c_s, wo, l)
        norm_rows(z, n_s, MG)
        for n in range(0, D, TN):
            qkv[0:MG, n:n + TN] = jnp.dot(n_s[...], cq[l, :, n:n + TN], preferred_element_type=F32).astype(BF16)

        def cross_row(r, _):
            kv_wait(l, r)
            sl = lax.rem(r, 2)
            length = plan[P_LEN + first_row(i) + r]
            mask = lax.broadcasted_iota(I32, (two, T_ENC), 1) < length
            vmask = lax.broadcasted_iota(I32, (T_ENC, 128), 0) < length
            rows = pl.ds(pl.multiple_of(r * T_DEC, 32), T_DEC)
            for p in range(PAIRS):
                cols = slice(p * 128, (p + 1) * 128)
                c_s[rows, cols] = attend_pair(qkv[rows, cols], kb[sl, :, cols], vb[sl, :, cols], mask, vmask)

            @pl.when(r + 2 < G)
            def _():
                kv_start(l, r + 2)

            return 0

        lax.fori_loop(0, G, cross_row, 0)
        for j in range(5, 8):
            need(j, l)
        add_to_z(c_s, co, l)
        norm_rows(z, n_s, MG)
        for n in range(0, FF, TF):
            u = jnp.dot(n_s[...], w1[l, :, n:n + TF], preferred_element_type=F32)
            inner[:, n:n + TF] = gelu(u).astype(BF16)
        add_to_z(inner, w2, l)
        return 0

    lax.fori_loop(0, 2, layer, 0)

    for r in range(G):
        out_copy(i, slot, r).start()

    @pl.when(i == groups - 1)
    def _():
        for r in range(G):
            out_copy(i, slot, r).wait()


def decode_half(half, plan, y_dec, kvs, weights, prev):
    hbm = pl.BlockSpec(memory_space=pl.ANY)
    vm = lambda *s: pltpu.VMEM(s, BF16)
    ins = [y_dec, *kvs, *weights] + ([prev] if half else [])
    return pl.pallas_call(
        functools.partial(dec_kernel, half),
        out_shape=jax.ShapeDtypeStruct((ROWS, T_DEC, D), BF16),
        grid_spec=pltpu.PrefetchScalarGridSpec(
            num_scalar_prefetch=1,
            grid=(HALF // G,),
            in_specs=[hbm] * len(ins),
            out_specs=hbm,
            scratch_shapes=[
                vm(2, MG, D), vm(MG, D), vm(MG + 64, 3 * D), vm(MG, D),
                vm(2, T_ENC, D), vm(2, T_ENC, D),
                vm(2, D, D), vm(2, D, D), vm(2, D, D), vm(2, D, D), vm(2, D, D), vm(2, D, D), vm(2, D, FF), vm(2, FF, D),
                pltpu.SemaphoreType.DMA((2,)), pltpu.SemaphoreType.DMA((2,)), pltpu.SemaphoreType.DMA((2, 2)),
                pltpu.SemaphoreType.DMA((8, 2)),
            ],
        ),
        input_output_aliases={len(ins): 0} if half else {},
        compiler_params=pltpu.CompilerParams(vmem_limit_bytes=VMEM_MAX, dimension_semantics=("arbitrary",)),
        cost_estimate=pl.CostEstimate(flops=90_000_000_000, bytes_accessed=100_000_000, transcendentals=0),
        name="decode",
    )(plan, *ins)


def solution(mesh):
    pair_size = mesh.shape["pair"]
    to_partner = [(source, (source + pair_size // 2) % pair_size) for source in range(pair_size)]
    row_spec = P(("data", "pair"))
    full_spec = P()

    def per_device(x_enc, enc_len, y_dec, enc_wq, enc_wk, enc_wv, enc_wo, enc_w1, enc_w2, dec_wq, dec_wk, dec_wv, dec_wo, crs_wq, crs_wk, crs_wv, crs_wo, dec_w1, dec_w2):
        flat = lambda w: w.reshape(2, D, D)
        plan = make_plan(enc_len)
        partner_plan = lax.ppermute(plan, "pair", to_partner)
        enc_weights = (enc_wq, enc_wk, enc_wv, flat(enc_wo), enc_w1, enc_w2)
        enc_out, base, h = [], 0, x_enc
        for bins in CHUNKS:
            h = encode_chunk(base, bins, plan, x_enc, enc_weights, h)
            enc_out.append(lax.ppermute(h, "pair", to_partner))
            base += bins
        dec_weights = (dec_wq, dec_wk, dec_wv, flat(dec_wo), crs_wq, flat(crs_wo), dec_w1, dec_w2)
        out, kvs, after = None, [], h
        for half in range(2):
            hs = enc_out[2:] if half else enc_out[:2]
            kvs += cross_keys(half * NB // 2, partner_plan, hs, crs_wk, crs_wv, after)
            out = decode_half(half, partner_plan, y_dec, kvs, dec_weights, out)
            after = out
        return out

    return jax.shard_map(per_device, mesh=mesh, in_specs=(row_spec, row_spec, row_spec) + (full_spec,) * 16, out_specs=row_spec, check_vma=False)
```

```python
import functools

import jax
import jax.numpy as jnp
from jax import lax
from jax.experimental import pallas as pl
from jax.experimental.pallas import tpu as pltpu
from jax.sharding import PartitionSpec as P

BF16 = jnp.bfloat16
F32 = jnp.float32
I32 = jnp.int32

ROWS = 32
T_ENC = 256
T_DEC = 96
D = 1024
FF = 2816
PAIRS = 8
BIN = 512
NB = ROWS * T_ENC // BIN
CHUNKS = (4, 4, 2, 2, 4)
TN = 256
TF = 256
NS = 128
UNIT = 16
SCALE = 64 ** -0.5 * 1.4426950408889634
VMEM_MAX = 64 * 2**20 - 2**17

P_ORDER, P_OFF, P_LEN, P_GLOB, P_START, P_NBINS = 0, 32, 64, 96, 128, 160


def plan_kernel(len_ref, rank_ref, plan_ref, free, count, rbin, roff, rk, order):
    def clear(i, _):
        free[i] = BIN // UNIT
        count[i] = 0
        order[rank_ref[i]] = i
        order[rank_ref[i + NB]] = i + NB
        return 0

    lax.fori_loop(0, NB, clear, 0, unroll=4)

    def by_rank(i, _):
        r = order[i]
        size = (len_ref[r] + UNIT - 1) // UNIT
        b = lax.while_loop(lambda b: free[b] < size, lambda b: b + 1, jnp.int32(0))
        left = free[b]
        rbin[r] = b
        roff[r] = BIN - left * UNIT
        rk[r] = count[b]
        free[b] = left - size
        count[b] = count[b] + 1
        return 0

    lax.fori_loop(0, ROWS, by_rank, 0)

    def starts(b, carry):
        total, nbins = carry
        plan_ref[P_START + b] = total
        c = count[b]
        return total + c, nbins + jnp.where(c > 0, 1, 0)

    total, nbins = lax.fori_loop(0, NB, starts, (jnp.int32(0), jnp.int32(0)))
    plan_ref[P_START + NB] = total

    plan_ref[P_NBINS] = nbins

    def place(r, _):
        b = rbin[r]
        pos = plan_ref[P_START + b] + rk[r]
        plan_ref[P_ORDER + pos] = r
        plan_ref[P_OFF + pos] = roff[r]
        plan_ref[P_LEN + pos] = len_ref[r]
        plan_ref[P_GLOB + pos] = b * BIN + roff[r]
        return 0

    lax.fori_loop(0, ROWS, place, 0, unroll=4)


def make_plan(enc_len):
    units = (enc_len + UNIT - 1) // UNIT
    at = jnp.arange(ROWS)
    before = (units[None, :] > units[:, None]) | ((units[None, :] == units[:, None]) & (at[None, :] < at[:, None]))
    rank = jnp.sum(before.astype(I32), axis=1)
    smem = pl.BlockSpec(memory_space=pltpu.SMEM)
    return pl.pallas_call(
        plan_kernel,
        out_shape=jax.ShapeDtypeStruct((256,), I32),
        in_specs=[smem, smem],
        out_specs=smem,
        scratch_shapes=[pltpu.SMEM((32,), I32) for _ in range(6)],
        name="plan",
    )(enc_len, rank)


def norm_rows(src, dst, rows):
    step = NS
    for m in range(0, rows, step):
        v = src[m:m + step, :].astype(F32)
        inv = lax.rsqrt(jnp.mean(v * v, axis=-1, keepdims=True) + 1e-6)
        dst[m:m + step, :] = (v * inv).astype(BF16)


def gelu(x):
    inner = x * (x * x * (0.044715 * 0.7978845608028654) + 0.7978845608028654)
    half = x * 0.5
    return half + half * jnp.tanh(inner)


def attend_pair(q, k, v, mask, vmask=None):
    tq, tk = q.shape[0], k.shape[0]
    lane = lax.broadcasted_iota(I32, (tq, 128), 1)
    low = (lane < 64)
    lowf = low.astype(F32).astype(BF16)
    q2 = jnp.concatenate([q * lowf, q * (1 - lowf)], axis=0)
    s = lax.dot_general(q2, k, (((1,), (1,)), ((), ())), preferred_element_type=F32)
    s = jnp.where(mask, s, -1e30)
    top = jnp.max(s, axis=-1, keepdims=True)
    e = jnp.exp2((s - top) * SCALE).astype(BF16)
    if vmask is not None:
        v = jnp.where(vmask, v, jnp.zeros_like(v))
    va = jnp.concatenate([v, jnp.ones_like(v)], axis=1)
    o = jnp.dot(e, va, preferred_element_type=F32)
    num = jnp.where(low, o[:tq, :128], o[tq:, :128])
    den = jnp.where(low, o[:tq, 128:], o[tq:, 128:])
    return (num / den).astype(BF16)


def enc_kernel(base, plan, x_hbm, wq_h, wk_h, wv_h, wo_h, w1_h, w2_h, after, out_ref,
               xb, n_s, q_s, k_s, v_s, c_s, inner, wq, wk, wv, wo, w1, w2, xsem, wsem):
    i = pl.program_id(0)
    b = base + i
    nbins = plan[P_NBINS]
    slot = lax.rem(i, 2)
    weights = [(wq_h, wq), (wk_h, wk), (wv_h, wv), (wo_h, wo), (w1_h, w1), (w2_h, w2)]

    def weight_copy(j, l):
        return pltpu.make_async_copy(weights[j][0].at[l], weights[j][1].at[l], wsem.at[j, l])

    def row_copies(bb, sl, start):
        def per_row(pos, _):
            row, off = plan[P_ORDER + pos], plan[P_OFF + pos]
            units = (plan[P_LEN + pos] + UNIT - 1) // UNIT
            for bit in (16, 8, 4, 2, 1):
                @pl.when((units & bit) != 0)
                def _():
                    at = (units & ~(2 * bit - 1)) * UNIT
                    cp = pltpu.make_async_copy(
                        x_hbm.at[row, pl.ds(pl.multiple_of(at, UNIT), bit * UNIT), :],
                        xb.at[sl, pl.ds(pl.multiple_of(off + at, UNIT), bit * UNIT), :],
                        xsem.at[sl])
                    if start:
                        cp.start()
                    else:
                        cp.wait()
            return 0

        lax.fori_loop(plan[P_START + bb], plan[P_START + bb + 1], per_row, 0)

    @pl.when(jnp.logical_and(i == 0, b < nbins))
    def _():
        row_copies(b, slot, True)
        for j in range(3):
            weight_copy(j, 0).start()
        tail = slice(BIN if base < NB // 2 else BIN // 2, BIN + T_ENC)
        for ref in (q_s, k_s, v_s):
            ref[tail, :] = jnp.zeros((tail.stop - tail.start, D), BF16)
        c_s[...] = jnp.zeros_like(c_s)

    @pl.when(jnp.logical_and(i + 1 < pl.num_programs(0), b + 1 < nbins))
    def _():
        row_copies(b + 1, 1 - slot, True)

    @pl.when(b >= nbins)
    def _():
        out_ref[...] = jnp.zeros_like(out_ref)

    @pl.when(b < nbins)
    def _():
        row_copies(b, slot, False)
        first, last = plan[P_START + b], plan[P_START + b + 1]
        used = plan[P_OFF + last - 1] + (plan[P_LEN + last - 1] + UNIT - 1) // UNIT * UNIT
        h = xb.at[slot]

        def zero_unit(u, _):
            h[pl.ds(pl.multiple_of(u * UNIT, UNIT), UNIT), :] = jnp.zeros((UNIT, D), BF16)
            return 0

        lax.fori_loop(used // UNIT, BIN // UNIT, zero_unit, 0)

        def need(now, l, later, last):
            @pl.when(i == 0)
            def _():
                for j in now:
                    weight_copy(j, l).wait()

            @pl.when(jnp.logical_and(i == 0, last - l > 0))
            def _():
                for j in later:
                    weight_copy(j, l + 2 - last).start()

        def layer(m, l, _):
            need((0, 1, 2), l, (3, 4, 5), 2)
            norm_rows(h, n_s, m)
            for w, dst in ((wq, q_s), (wk, k_s), (wv, v_s)):
                for n in range(0, D, TN):
                    dst[0:m, n:n + TN] = jnp.dot(n_s[0:m, :], w[l, :, n:n + TN], preferred_element_type=F32).astype(BF16)

            def per_row(pos, _):
                off = pl.multiple_of(plan[P_OFF + pos], UNIT)
                length = plan[P_LEN + pos]

                def run(t):
                    mask = lax.broadcasted_iota(I32, (2 * t, T_ENC), 1) < length
                    for p in range(PAIRS):
                        cols = slice(p * 128, (p + 1) * 128)
                        c_s[pl.ds(off, t), cols] = attend_pair(
                            q_s[pl.ds(off, t), cols], k_s[pl.ds(off, T_ENC), cols], v_s[pl.ds(off, T_ENC), cols], mask)

                for t in range(96, T_ENC + 1, 32):
                    lo = 0 if t == 96 else t - 32

                    @pl.when(jnp.logical_and(length > lo, length <= t))
                    def _():
                        run(t)

                return 0

            lax.fori_loop(first, last, per_row, 0)
            need((3, 4, 5), l, (0, 1, 2), 1)
            for n in range(0, D, TN):
                u = jnp.dot(c_s[0:m, :], wo[l, :, n:n + TN], preferred_element_type=F32)
                h[0:m, n:n + TN] = (h[0:m, n:n + TN].astype(F32) + u).astype(BF16)
            norm_rows(h, n_s, m)
            for n in range(0, FF, TF):
                u = jnp.dot(n_s[0:m, :], w1[l, :, n:n + TF], preferred_element_type=F32)
                inner[0:m, n:n + TF] = gelu(u).astype(BF16)
            for n in range(0, D, TN):
                u = jnp.dot(inner[0:m, :], w2[l, :, n:n + TN], preferred_element_type=F32)
                h[0:m, n:n + TN] = (h[0:m, n:n + TN].astype(F32) + u).astype(BF16)
            return 0

        if base < NB // 2:
            lax.fori_loop(0, 2, functools.partial(layer, BIN), 0)
        else:
            @pl.when(used > BIN // 2)
            def _():
                lax.fori_loop(0, 2, functools.partial(layer, BIN), 0)

            @pl.when(used <= BIN // 2)
            def _():
                lax.fori_loop(0, 2, functools.partial(layer, BIN // 2), 0)

        norm_rows(h, out_ref, BIN)


def encode_chunk(base, bins, plan, x_enc, weights, after):
    hbm = pl.BlockSpec(memory_space=pl.ANY)
    vm = lambda *s: pltpu.VMEM(s, BF16)
    tokens = BIN + T_ENC
    return pl.pallas_call(
        functools.partial(enc_kernel, base),
        out_shape=jax.ShapeDtypeStruct((bins * BIN, D), BF16),
        grid_spec=pltpu.PrefetchScalarGridSpec(
            num_scalar_prefetch=1,
            grid=(bins,),
            in_specs=[hbm] * 8,
            out_specs=pl.BlockSpec((BIN, D), lambda i, plan: (i, 0)),
            scratch_shapes=[
                vm(2, BIN, D), vm(BIN, D), vm(tokens, D), vm(tokens, D), vm(tokens, D), vm(tokens, D), vm(BIN, FF),
                vm(2, D, D), vm(2, D, D), vm(2, D, D), vm(2, D, D), vm(2, D, FF), vm(2, FF, D),
                pltpu.SemaphoreType.DMA((2,)), pltpu.SemaphoreType.DMA((6, 2)),
            ],
        ),
        compiler_params=pltpu.CompilerParams(vmem_limit_bytes=VMEM_MAX, dimension_semantics=("arbitrary",)),
        cost_estimate=pl.CostEstimate(flops=20_000_000_000 * bins, bytes_accessed=60_000_000, transcendentals=0),
        name="encode",
    )(plan, x_enc, *weights, after)


def cross_kernel(base, sizes, plan, *refs):
    h_hbm = refs[:len(sizes)]
    wk_h, wv_h, after, k_ref, v_ref, hb, wk_s, wv_s, hsem, wsem = refs[len(sizes):]
    i = pl.program_id(0)
    slot = lax.rem(i, 2)
    nbins = plan[P_NBINS] - base

    def fetch(at, sl, start):
        lo = 0
        for ref, size in zip(h_hbm, sizes):
            @pl.when(jnp.logical_and(at < nbins, jnp.logical_and(at >= lo, at < lo + size)))
            def _(ref=ref, lo=lo):
                cp = pltpu.make_async_copy(
                    ref.at[pl.ds(pl.multiple_of((at - lo) * BIN, BIN), BIN), :], hb.at[sl], hsem.at[sl])
                if start:
                    cp.start()
                else:
                    cp.wait()
            lo += size

    def weight_copy(t):
        src, dst = ((wk_h, wk_s), (wv_h, wv_s))[t % 2]
        return pltpu.make_async_copy(src.at[t // 2], dst.at[t // 2], wsem.at[t])

    @pl.when(i == 0)
    def _():
        fetch(i, slot, True)

    @pl.when(jnp.logical_and(i == 0, nbins > 0))
    def _():
        weight_copy(0).start()

    @pl.when(i + 1 < sum(sizes))
    def _():
        fetch(i + 1, 1 - slot, True)

    fetch(i, slot, False)

    @pl.when(i < nbins)
    def _():
        for l in range(2):
            for w, dst in ((wk_s, k_ref), (wv_s, v_ref)):
                t = 2 * l + (dst is v_ref)

                @pl.when(i == 0)
                def _(t=t):
                    weight_copy(t).wait()
                    if t < 3:
                        weight_copy(t + 1).start()

                for n in range(0, D, TN):
                    dst[l, :, n:n + TN] = jnp.dot(hb[slot], w[l, :, n:n + TN], preferred_element_type=F32).astype(BF16)


def cross_keys(base, plan, hs, wk, wv, after):
    sizes = tuple(h.shape[0] // BIN for h in hs)
    tokens = sum(sizes) * BIN
    hbm = pl.BlockSpec(memory_space=pl.ANY)

    def block(i, plan):
        return 0, jnp.minimum(i, jnp.maximum(plan[P_NBINS] - 1 - base, 0)), 0

    spec = pl.BlockSpec((2, BIN, D), block)
    return pl.pallas_call(
        functools.partial(cross_kernel, base, sizes),
        out_shape=[jax.ShapeDtypeStruct((2, tokens + BIN, D), BF16)] * 2,
        grid_spec=pltpu.PrefetchScalarGridSpec(
            num_scalar_prefetch=1, grid=(sum(sizes),), in_specs=[hbm] * (len(hs) + 3), out_specs=[spec] * 2,
            scratch_shapes=[pltpu.VMEM((2, BIN, D), BF16), pltpu.VMEM((2, D, D), BF16), pltpu.VMEM((2, D, D), BF16),
                            pltpu.SemaphoreType.DMA((2,)), pltpu.SemaphoreType.DMA((4,))]),
        compiler_params=pltpu.CompilerParams(vmem_limit_bytes=VMEM_MAX, dimension_semantics=("arbitrary",)),
        cost_estimate=pl.CostEstimate(flops=8 * tokens * D * D, bytes_accessed=10 * tokens * D, transcendentals=0),
        name="cross_keys",
    )(plan, *hs, wk, wv, after)


G = 8
MG = G * T_DEC
HALF = ROWS // 2
HALF_TOKENS = NB * BIN // 2


def dec_kernel(half, plan, *refs):
    nkv = half + 1
    y_hbm = refs[0]
    kv_hbm = refs[1:1 + 2 * nkv]
    w_hbm = refs[1 + 2 * nkv:9 + 2 * nkv]
    rest = refs[9 + 2 * nkv + (1 if half else 0):]
    out_hbm, zb, n_s, qkv, c_s, kb, vb = rest[:7]
    w_s = rest[7:15]
    ysem, osem, kvsem, wsem = rest[15:]
    inner = qkv.at[0:MG, 0:FF]
    wq, wk, wv, wo, cq, co, w1, w2 = w_s
    i = pl.program_id(0)
    groups = pl.num_programs(0)
    slot = lax.rem(i, 2)

    def weight_copy(j, l):
        return pltpu.make_async_copy(w_hbm[j].at[l], w_s[j].at[l], wsem.at[j, l])

    def first_row(g):
        return half * HALF + g * G

    def y_copy(g, sl, r):
        row = plan[P_ORDER + first_row(g) + r]
        return pltpu.make_async_copy(y_hbm.at[row], zb.at[sl, pl.ds(r * T_DEC, T_DEC), :], ysem.at[sl])

    def out_copy(g, sl, r):
        row = plan[P_ORDER + first_row(g) + r]
        return pltpu.make_async_copy(zb.at[sl, pl.ds(r * T_DEC, T_DEC), :], out_hbm.at[row], osem.at[sl])

    def kv_start(l, r):
        at = plan[P_GLOB + first_row(i) + r]
        sl = lax.rem(r, 2)
        for part in range(nkv):
            @pl.when(jnp.logical_and(at >= part * HALF_TOKENS, at < (part + 1) * HALF_TOKENS))
            def _():
                rows = pl.ds(pl.multiple_of(at - part * HALF_TOKENS, UNIT), T_ENC)
                pltpu.make_async_copy(kv_hbm[2 * part].at[l, rows, :], kb.at[sl], kvsem.at[0, sl]).start()
                pltpu.make_async_copy(kv_hbm[2 * part + 1].at[l, rows, :], vb.at[sl], kvsem.at[1, sl]).start()

    def kv_wait(l, r):
        sl = lax.rem(r, 2)
        pltpu.make_async_copy(kv_hbm[0].at[l, pl.ds(0, T_ENC), :], kb.at[sl], kvsem.at[0, sl]).wait()
        pltpu.make_async_copy(kv_hbm[1].at[l, pl.ds(0, T_ENC), :], vb.at[sl], kvsem.at[1, sl]).wait()

    @pl.when(i == 0)
    def _():
        qkv[MG:MG + 64, :] = jnp.zeros((64, 3 * D), BF16)
        for r in range(G):
            y_copy(0, 0, r).start()
        for j in range(3):
            weight_copy(j, 0).start()

    @pl.when(i >= 1)
    def _():
        for r in range(G):
            out_copy(i - 1, 1 - slot, r).wait()

    @pl.when(i + 1 < groups)
    def _():
        for r in range(G):
            y_copy(i + 1, 1 - slot, r).start()

    for r in range(G):
        y_copy(i, slot, r).wait()
    z = zb.at[slot]

    def need(now, l, later, last):
        @pl.when(i == 0)
        def _():
            for j in now:
                weight_copy(j, l).wait()

        @pl.when(jnp.logical_and(i == 0, last - l > 0))
        def _():
            for j in later:
                weight_copy(j, l + 2 - last).start()

    def add_to_z(src, w, l):
        for n in range(0, D, TN):
            u = jnp.dot(src[...], w[l, :, n:n + TN], preferred_element_type=F32)
            z[:, n:n + TN] = (z[:, n:n + TN].astype(F32) + u).astype(BF16)

    def layer(l, _):
        kv_start(l, jnp.int32(0))
        kv_start(l, jnp.int32(1))
        need((0, 1, 2), l, (3, 4), 2)
        norm_rows(z, n_s, MG)
        for j, w in enumerate((wq, wk, wv)):
            for n in range(0, D, TN):
                qkv[0:MG, j * D + n:j * D + n + TN] = jnp.dot(n_s[...], w[l, :, n:n + TN], preferred_element_type=F32).astype(BF16)
        two = 2 * T_DEC
        row_at = lax.broadcasted_iota(I32, (2 * two, T_ENC), 0)
        row_at = jnp.where(row_at >= two, row_at - two, row_at)
        col_at = lax.broadcasted_iota(I32, (2 * two, T_ENC), 1)
        causal = (row_at >= col_at) & ((row_at < T_DEC) | (col_at >= T_DEC))

        def self_rows(r, _):
            at = pl.multiple_of(r * two, 64)
            for p in range(PAIRS):
                cols = slice(p * 128, (p + 1) * 128)
                c_s[pl.ds(at, two), cols] = attend_pair(
                    qkv[pl.ds(at, two), p * 128:(p + 1) * 128],
                    qkv[pl.ds(at, T_ENC), D + p * 128:D + (p + 1) * 128],
                    qkv[pl.ds(at, T_ENC), 2 * D + p * 128:2 * D + (p + 1) * 128], causal)
            return 0

        lax.fori_loop(0, G // 2, self_rows, 0)
        need((3, 4), l, (5, 6, 7), 2)
        add_to_z(c_s, wo, l)
        norm_rows(z, n_s, MG)
        for n in range(0, D, TN):
            qkv[0:MG, n:n + TN] = jnp.dot(n_s[...], cq[l, :, n:n + TN], preferred_element_type=F32).astype(BF16)

        def cross_row(r, _):
            kv_wait(l, r)
            sl = lax.rem(r, 2)
            length = plan[P_LEN + first_row(i) + r]
            mask = lax.broadcasted_iota(I32, (two, T_ENC), 1) < length
            vmask = lax.broadcasted_iota(I32, (T_ENC, 128), 0) < length
            rows = pl.ds(pl.multiple_of(r * T_DEC, 32), T_DEC)
            for p in range(PAIRS):
                cols = slice(p * 128, (p + 1) * 128)
                c_s[rows, cols] = attend_pair(qkv[rows, cols], kb[sl, :, cols], vb[sl, :, cols], mask, vmask)

            @pl.when(r + 2 < G)
            def _():
                kv_start(l, r + 2)

            return 0

        lax.fori_loop(0, G, cross_row, 0)
        need((5, 6, 7), l, (0, 1, 2), 1)
        add_to_z(c_s, co, l)
        norm_rows(z, n_s, MG)
        for n in range(0, FF, TF):
            u = jnp.dot(n_s[...], w1[l, :, n:n + TF], preferred_element_type=F32)
            inner[:, n:n + TF] = gelu(u).astype(BF16)
        add_to_z(inner, w2, l)
        return 0

    lax.fori_loop(0, 2, layer, 0)

    for r in range(G):
        out_copy(i, slot, r).start()

    @pl.when(i == groups - 1)
    def _():
        for r in range(G):
            out_copy(i, slot, r).wait()


def decode_half(half, plan, y_dec, kvs, weights, prev):
    hbm = pl.BlockSpec(memory_space=pl.ANY)
    vm = lambda *s: pltpu.VMEM(s, BF16)
    ins = [y_dec, *kvs, *weights] + ([prev] if half else [])
    return pl.pallas_call(
        functools.partial(dec_kernel, half),
        out_shape=jax.ShapeDtypeStruct((ROWS, T_DEC, D), BF16),
        grid_spec=pltpu.PrefetchScalarGridSpec(
            num_scalar_prefetch=1,
            grid=(HALF // G,),
            in_specs=[hbm] * len(ins),
            out_specs=hbm,
            scratch_shapes=[
                vm(2, MG, D), vm(MG, D), vm(MG + 64, 3 * D), vm(MG, D),
                vm(2, T_ENC, D), vm(2, T_ENC, D),
                vm(2, D, D), vm(2, D, D), vm(2, D, D), vm(2, D, D), vm(2, D, D), vm(2, D, D), vm(2, D, FF), vm(2, FF, D),
                pltpu.SemaphoreType.DMA((2,)), pltpu.SemaphoreType.DMA((2,)), pltpu.SemaphoreType.DMA((2, 2)),
                pltpu.SemaphoreType.DMA((8, 2)),
            ],
        ),
        input_output_aliases={len(ins): 0} if half else {},
        compiler_params=pltpu.CompilerParams(vmem_limit_bytes=VMEM_MAX, dimension_semantics=("arbitrary",)),
        cost_estimate=pl.CostEstimate(flops=90_000_000_000, bytes_accessed=100_000_000, transcendentals=0),
        name="decode",
    )(plan, *ins)


def solution(mesh):
    pair_size = mesh.shape["pair"]
    to_partner = [(source, (source + pair_size // 2) % pair_size) for source in range(pair_size)]
    row_spec = P(("data", "pair"))
    full_spec = P()

    def per_device(x_enc, enc_len, y_dec, enc_wq, enc_wk, enc_wv, enc_wo, enc_w1, enc_w2, dec_wq, dec_wk, dec_wv, dec_wo, crs_wq, crs_wk, crs_wv, crs_wo, dec_w1, dec_w2):
        flat = lambda w: w.reshape(2, D, D)
        plan = make_plan(enc_len)
        partner_plan = lax.ppermute(plan, "pair", to_partner)
        enc_weights = (enc_wq, enc_wk, enc_wv, flat(enc_wo), enc_w1, enc_w2)
        enc_out, base, h = [], 0, x_enc
        for bins in CHUNKS:
            h = encode_chunk(base, bins, plan, x_enc, enc_weights, h)
            enc_out.append(lax.ppermute(h, "pair", to_partner))
            base += bins
        dec_weights = (dec_wq, dec_wk, dec_wv, flat(dec_wo), crs_wq, flat(crs_wo), dec_w1, dec_w2)
        out, kvs, after = None, [], h
        for half in range(2):
            hs = enc_out[2:] if half else enc_out[:2]
            kvs += cross_keys(half * NB // 2, partner_plan, hs, crs_wk, crs_wv, after)
            out = decode_half(half, partner_plan, y_dec, kvs, dec_weights, out)
            after = out
        return out

    return jax.shard_map(per_device, mesh=mesh, in_specs=(row_spec, row_spec, row_spec) + (full_spec,) * 16, out_specs=row_spec, check_vma=False)
```

```python
import functools

import jax
import jax.numpy as jnp
from jax import lax
from jax.experimental import pallas as pl
from jax.experimental.pallas import tpu as pltpu
from jax.sharding import PartitionSpec as P

BF16 = jnp.bfloat16
F32 = jnp.float32
I32 = jnp.int32

ROWS = 32
T_ENC = 256
T_DEC = 96
D = 1024
FF = 2816
PAIRS = 8
BIN = 512
NB = ROWS * T_ENC // BIN
CHUNKS = (4, 4, 8)
BUCKETS = (96, 128, 160, 192, 224, 256)
TN = 256
TF = 256
NS = 128
UNIT = 16
SCALE = 64 ** -0.5 * 1.4426950408889634
VMEM_MAX = 64 * 2**20 - 2**17

P_ORDER, P_OFF, P_LEN, P_GLOB, P_START, P_NBINS = 0, 32, 64, 96, 128, 160


def plan_kernel(len_ref, rank_ref, plan_ref, free, count, rbin, roff, rk, order):
    def clear(i, _):
        free[i] = BIN // UNIT
        count[i] = 0
        order[rank_ref[i]] = i
        order[rank_ref[i + NB]] = i + NB
        return 0

    lax.fori_loop(0, NB, clear, 0, unroll=4)

    def by_rank(i, _):
        r = order[i]
        size = (len_ref[r] + UNIT - 1) // UNIT
        b = lax.while_loop(lambda b: free[b] < size, lambda b: b + 1, jnp.int32(0))
        left = free[b]
        rbin[r] = b
        roff[r] = BIN - left * UNIT
        rk[r] = count[b]
        free[b] = left - size
        count[b] = count[b] + 1
        return 0

    lax.fori_loop(0, ROWS, by_rank, 0)

    def starts(b, carry):
        total, nbins = carry
        plan_ref[P_START + b] = total
        c = count[b]
        return total + c, nbins + jnp.where(c > 0, 1, 0)

    total, nbins = lax.fori_loop(0, NB, starts, (jnp.int32(0), jnp.int32(0)))
    plan_ref[P_START + NB] = total

    plan_ref[P_NBINS] = nbins

    def place(r, _):
        b = rbin[r]
        pos = plan_ref[P_START + b] + rk[r]
        plan_ref[P_ORDER + pos] = r
        plan_ref[P_OFF + pos] = roff[r]
        plan_ref[P_LEN + pos] = len_ref[r]
        plan_ref[P_GLOB + pos] = b * BIN + roff[r]
        return 0

    lax.fori_loop(0, ROWS, place, 0, unroll=4)


def make_plan(enc_len):
    units = (enc_len + UNIT - 1) // UNIT
    at = jnp.arange(ROWS)
    before = (units[None, :] > units[:, None]) | ((units[None, :] == units[:, None]) & (at[None, :] < at[:, None]))
    rank = jnp.sum(before.astype(I32), axis=1)
    smem = pl.BlockSpec(memory_space=pltpu.SMEM)
    return pl.pallas_call(
        plan_kernel,
        out_shape=jax.ShapeDtypeStruct((256,), I32),
        in_specs=[smem, smem],
        out_specs=smem,
        scratch_shapes=[pltpu.SMEM((32,), I32) for _ in range(6)],
        name="plan",
    )(enc_len, rank)


def norm_rows(src, dst, rows):
    step = NS
    for m in range(0, rows, step):
        v = src[m:m + step, :].astype(F32)
        inv = lax.rsqrt(jnp.mean(v * v, axis=-1, keepdims=True) + 1e-6)
        dst[m:m + step, :] = (v * inv).astype(BF16)


def gelu(x):
    inner = x * (x * x * (0.044715 * 0.7978845608028654) + 0.7978845608028654)
    half = x * 0.5
    return half + half * jnp.tanh(inner)


def attend_pair(q, k, v, mask, vmask=None):
    tq, tk = q.shape[0], k.shape[0]
    lane = lax.broadcasted_iota(I32, (tq, 128), 1)
    low = (lane < 64)
    lowf = low.astype(F32).astype(BF16)
    q2 = jnp.concatenate([q * lowf, q * (1 - lowf)], axis=0)
    s = lax.dot_general(q2, k, (((1,), (1,)), ((), ())), preferred_element_type=F32)
    s = jnp.where(mask, s, -1e30)
    top = jnp.max(s, axis=-1, keepdims=True)
    e = jnp.exp2((s - top) * SCALE).astype(BF16)
    if vmask is not None:
        v = jnp.where(vmask, v, jnp.zeros_like(v))
    va = jnp.concatenate([v, jnp.ones_like(v)], axis=1)
    o = jnp.dot(e, va, preferred_element_type=F32)
    num = jnp.where(low, o[:tq, :128], o[tq:, :128])
    den = jnp.where(low, o[:tq, 128:], o[tq:, 128:])
    return (num / den).astype(BF16)


def enc_kernel(base, plan, x_hbm, wq_h, wk_h, wv_h, wo_h, w1_h, w2_h, after, out_ref,
               xb, n_s, q_s, k_s, v_s, c_s, inner, wq, wk, wv, wo, w1, w2, xsem, wsem):
    i = pl.program_id(0)
    b = base + i
    nbins = plan[P_NBINS]
    slot = lax.rem(i, 2)
    weights = [(wq_h, wq), (wk_h, wk), (wv_h, wv), (wo_h, wo), (w1_h, w1), (w2_h, w2)]

    def weight_copy(j, l):
        return pltpu.make_async_copy(weights[j][0].at[l], weights[j][1].at[l], wsem.at[j, l])

    def row_copies(bb, sl, start):
        def per_row(pos, _):
            row, off = plan[P_ORDER + pos], plan[P_OFF + pos]
            units = (plan[P_LEN + pos] + UNIT - 1) // UNIT
            for bit in (16, 8, 4, 2, 1):
                @pl.when((units & bit) != 0)
                def _():
                    at = (units & ~(2 * bit - 1)) * UNIT
                    cp = pltpu.make_async_copy(
                        x_hbm.at[row, pl.ds(pl.multiple_of(at, UNIT), bit * UNIT), :],
                        xb.at[sl, pl.ds(pl.multiple_of(off + at, UNIT), bit * UNIT), :],
                        xsem.at[sl])
                    if start:
                        cp.start()
                    else:
                        cp.wait()
            return 0

        lax.fori_loop(plan[P_START + bb], plan[P_START + bb + 1], per_row, 0)

    @pl.when(jnp.logical_and(i == 0, b < nbins))
    def _():
        row_copies(b, slot, True)
        for l in range(2):
            for j in range(6):
                weight_copy(j, l).start()
        tail = slice(BIN, BIN + T_ENC)
        for ref in (q_s, k_s, v_s):
            ref[tail, :] = jnp.zeros((T_ENC, D), BF16)
        c_s[...] = jnp.zeros_like(c_s)

    @pl.when(jnp.logical_and(i + 1 < pl.num_programs(0), b + 1 < nbins))
    def _():
        row_copies(b + 1, 1 - slot, True)

    @pl.when(b >= nbins)
    def _():
        out_ref[...] = jnp.zeros_like(out_ref)

    @pl.when(b < nbins)
    def _():
        row_copies(b, slot, False)
        first, last = plan[P_START + b], plan[P_START + b + 1]
        used = plan[P_OFF + last - 1] + (plan[P_LEN + last - 1] + UNIT - 1) // UNIT * UNIT
        h = xb.at[slot]

        def zero_unit(u, _):
            h[pl.ds(pl.multiple_of(u * UNIT, UNIT), UNIT), :] = jnp.zeros((UNIT, D), BF16)
            return 0

        lax.fori_loop(used // UNIT, BIN // UNIT, zero_unit, 0)

        def need(j, l):
            @pl.when(i == 0)
            def _():
                weight_copy(j, l).wait()

        def layer(l, _):
            for j in range(3):
                need(j, l)
            norm_rows(h, n_s, BIN)
            for w, dst in ((wq, q_s), (wk, k_s), (wv, v_s)):
                for n in range(0, D, TN):
                    dst[0:BIN, n:n + TN] = jnp.dot(n_s[...], w[l, :, n:n + TN], preferred_element_type=F32).astype(BF16)

            def per_row(pos, _):
                off = pl.multiple_of(plan[P_OFF + pos], UNIT)
                length = plan[P_LEN + pos]

                def run(t):
                    mask = lax.broadcasted_iota(I32, (2 * t, T_ENC), 1) < length
                    for p in range(PAIRS):
                        cols = slice(p * 128, (p + 1) * 128)
                        c_s[pl.ds(off, t), cols] = attend_pair(
                            q_s[pl.ds(off, t), cols], k_s[pl.ds(off, T_ENC), cols], v_s[pl.ds(off, T_ENC), cols], mask)

                for lo, t in zip((0,) + BUCKETS, BUCKETS):
                    @pl.when(jnp.logical_and(length > lo, length <= t))
                    def _():
                        run(t)

                return 0

            lax.fori_loop(first, last, per_row, 0)
            for j in range(3, 6):
                need(j, l)
            for n in range(0, D, TN):
                u = jnp.dot(c_s[0:BIN, :], wo[l, :, n:n + TN], preferred_element_type=F32)
                h[:, n:n + TN] = (h[:, n:n + TN].astype(F32) + u).astype(BF16)
            norm_rows(h, n_s, BIN)
            for n in range(0, FF, TF):
                u = jnp.dot(n_s[...], w1[l, :, n:n + TF], preferred_element_type=F32)
                inner[:, n:n + TF] = gelu(u).astype(BF16)
            for n in range(0, D, TN):
                u = jnp.dot(inner[...], w2[l, :, n:n + TN], preferred_element_type=F32)
                h[:, n:n + TN] = (h[:, n:n + TN].astype(F32) + u).astype(BF16)
            return 0

        lax.fori_loop(0, 2, layer, 0)
        norm_rows(h, out_ref, BIN)


def encode_chunk(base, bins, plan, x_enc, weights, after):
    hbm = pl.BlockSpec(memory_space=pl.ANY)
    vm = lambda *s: pltpu.VMEM(s, BF16)
    tokens = BIN + T_ENC
    return pl.pallas_call(
        functools.partial(enc_kernel, base),
        out_shape=jax.ShapeDtypeStruct((bins * BIN, D), BF16),
        grid_spec=pltpu.PrefetchScalarGridSpec(
            num_scalar_prefetch=1,
            grid=(bins,),
            in_specs=[hbm] * 8,
            out_specs=pl.BlockSpec((BIN, D), lambda i, plan: (i, 0)),
            scratch_shapes=[
                vm(2, BIN, D), vm(BIN, D), vm(tokens, D), vm(tokens, D), vm(tokens, D), vm(tokens, D), vm(BIN, FF),
                vm(2, D, D), vm(2, D, D), vm(2, D, D), vm(2, D, D), vm(2, D, FF), vm(2, FF, D),
                pltpu.SemaphoreType.DMA((2,)), pltpu.SemaphoreType.DMA((6, 2)),
            ],
        ),
        compiler_params=pltpu.CompilerParams(vmem_limit_bytes=VMEM_MAX, dimension_semantics=("arbitrary",)),
        cost_estimate=pl.CostEstimate(flops=20_000_000_000 * bins, bytes_accessed=60_000_000, transcendentals=0),
        name="encode",
    )(plan, x_enc, *weights, after)


def cross_kernel(base, sizes, plan, *refs):
    h_hbm = refs[:len(sizes)]
    wk_ref, wv_ref, after, k_ref, v_ref, hb, hsem = refs[len(sizes):]
    i = pl.program_id(0)
    slot = lax.rem(i, 2)
    nbins = plan[P_NBINS] - base

    def fetch(at, sl, start):
        lo = 0
        for ref, size in zip(h_hbm, sizes):
            @pl.when(jnp.logical_and(at < nbins, jnp.logical_and(at >= lo, at < lo + size)))
            def _(ref=ref, lo=lo):
                cp = pltpu.make_async_copy(
                    ref.at[pl.ds(pl.multiple_of((at - lo) * BIN, BIN), BIN), :], hb.at[sl], hsem.at[sl])
                if start:
                    cp.start()
                else:
                    cp.wait()
            lo += size

    @pl.when(i == 0)
    def _():
        fetch(i, slot, True)

    @pl.when(i + 1 < sum(sizes))
    def _():
        fetch(i + 1, 1 - slot, True)

    fetch(i, slot, False)

    @pl.when(i < nbins)
    def _():
        for l in range(2):
            for w, dst in ((wk_ref, k_ref), (wv_ref, v_ref)):
                for n in range(0, D, TN):
                    dst[l, :, n:n + TN] = jnp.dot(hb[slot], w[l, :, n:n + TN], preferred_element_type=F32).astype(BF16)


def cross_keys(base, plan, hs, wk, wv, after):
    sizes = tuple(h.shape[0] // BIN for h in hs)
    tokens = sum(sizes) * BIN
    hbm = pl.BlockSpec(memory_space=pl.ANY)
    whole = pl.BlockSpec((2, D, D), lambda i, plan: (0, 0, 0))

    def block(i, plan):
        return 0, jnp.minimum(i, jnp.maximum(plan[P_NBINS] - 1 - base, 0)), 0

    spec = pl.BlockSpec((2, BIN, D), block)
    return pl.pallas_call(
        functools.partial(cross_kernel, base, sizes),
        out_shape=[jax.ShapeDtypeStruct((2, tokens + BIN, D), BF16)] * 2,
        grid_spec=pltpu.PrefetchScalarGridSpec(
            num_scalar_prefetch=1, grid=(sum(sizes),), in_specs=[hbm] * len(hs) + [whole, whole, hbm], out_specs=[spec] * 2,
            scratch_shapes=[pltpu.VMEM((2, BIN, D), BF16), pltpu.SemaphoreType.DMA((2,))]),
        compiler_params=pltpu.CompilerParams(vmem_limit_bytes=VMEM_MAX, dimension_semantics=("arbitrary",)),
        cost_estimate=pl.CostEstimate(flops=8 * tokens * D * D, bytes_accessed=10 * tokens * D, transcendentals=0),
        name="cross_keys",
    )(plan, *hs, wk, wv, after)


G = 8
MG = G * T_DEC
HALF = ROWS // 2
HALF_TOKENS = NB * BIN // 2


def dec_kernel(half, plan, *refs):
    nkv = half + 1
    y_hbm = refs[0]
    kv_hbm = refs[1:1 + 2 * nkv]
    w_hbm = refs[1 + 2 * nkv:9 + 2 * nkv]
    rest = refs[9 + 2 * nkv + (1 if half else 0):]
    out_hbm, zb, n_s, qkv, c_s, kb, vb = rest[:7]
    w_s = rest[7:15]
    ysem, osem, kvsem, wsem = rest[15:]
    inner = qkv.at[0:MG, 0:FF]
    wq, wk, wv, wo, cq, co, w1, w2 = w_s
    i = pl.program_id(0)
    groups = pl.num_programs(0)
    slot = lax.rem(i, 2)

    def weight_copy(j, l):
        return pltpu.make_async_copy(w_hbm[j].at[l], w_s[j].at[l], wsem.at[j, l])

    def first_row(g):
        return half * HALF + g * G

    def y_copy(g, sl, r):
        row = plan[P_ORDER + first_row(g) + r]
        return pltpu.make_async_copy(y_hbm.at[row], zb.at[sl, pl.ds(r * T_DEC, T_DEC), :], ysem.at[sl])

    def out_copy(g, sl, r):
        row = plan[P_ORDER + first_row(g) + r]
        return pltpu.make_async_copy(zb.at[sl, pl.ds(r * T_DEC, T_DEC), :], out_hbm.at[row], osem.at[sl])

    def kv_start(l, r):
        at = plan[P_GLOB + first_row(i) + r]
        sl = lax.rem(r, 2)
        for part in range(nkv):
            @pl.when(jnp.logical_and(at >= part * HALF_TOKENS, at < (part + 1) * HALF_TOKENS))
            def _():
                rows = pl.ds(pl.multiple_of(at - part * HALF_TOKENS, UNIT), T_ENC)
                pltpu.make_async_copy(kv_hbm[2 * part].at[l, rows, :], kb.at[sl], kvsem.at[0, sl]).start()
                pltpu.make_async_copy(kv_hbm[2 * part + 1].at[l, rows, :], vb.at[sl], kvsem.at[1, sl]).start()

    def kv_wait(l, r):
        sl = lax.rem(r, 2)
        pltpu.make_async_copy(kv_hbm[0].at[l, pl.ds(0, T_ENC), :], kb.at[sl], kvsem.at[0, sl]).wait()
        pltpu.make_async_copy(kv_hbm[1].at[l, pl.ds(0, T_ENC), :], vb.at[sl], kvsem.at[1, sl]).wait()

    @pl.when(i == 0)
    def _():
        qkv[MG:MG + 64, :] = jnp.zeros((64, 3 * D), BF16)
        for r in range(G):
            y_copy(0, 0, r).start()
        for j in range(3):
            weight_copy(j, 0).start()

    @pl.when(i >= 1)
    def _():
        for r in range(G):
            out_copy(i - 1, 1 - slot, r).wait()

    @pl.when(i + 1 < groups)
    def _():
        for r in range(G):
            y_copy(i + 1, 1 - slot, r).start()

    for r in range(G):
        y_copy(i, slot, r).wait()
    z = zb.at[slot]

    def need(now, l, later, last):
        @pl.when(i == 0)
        def _():
            for j in now:
                weight_copy(j, l).wait()

        @pl.when(jnp.logical_and(i == 0, last - l > 0))
        def _():
            for j in later:
                weight_copy(j, l + 2 - last).start()

    def add_to_z(src, w, l):
        for n in range(0, D, TN):
            u = jnp.dot(src[...], w[l, :, n:n + TN], preferred_element_type=F32)
            z[:, n:n + TN] = (z[:, n:n + TN].astype(F32) + u).astype(BF16)

    def layer(l, _):
        kv_start(l, jnp.int32(0))
        kv_start(l, jnp.int32(1))
        need((0, 1, 2), l, (3, 4), 2)
        norm_rows(z, n_s, MG)
        for j, w in enumerate((wq, wk, wv)):
            for n in range(0, D, TN):
                qkv[0:MG, j * D + n:j * D + n + TN] = jnp.dot(n_s[...], w[l, :, n:n + TN], preferred_element_type=F32).astype(BF16)
        two = 2 * T_DEC
        row_at = lax.broadcasted_iota(I32, (2 * two, T_ENC), 0)
        row_at = jnp.where(row_at >= two, row_at - two, row_at)
        col_at = lax.broadcasted_iota(I32, (2 * two, T_ENC), 1)
        causal = (row_at >= col_at) & ((row_at < T_DEC) | (col_at >= T_DEC))

        def self_rows(r, _):
            at = pl.multiple_of(r * two, 64)
            for p in range(PAIRS):
                cols = slice(p * 128, (p + 1) * 128)
                c_s[pl.ds(at, two), cols] = attend_pair(
                    qkv[pl.ds(at, two), p * 128:(p + 1) * 128],
                    qkv[pl.ds(at, T_ENC), D + p * 128:D + (p + 1) * 128],
                    qkv[pl.ds(at, T_ENC), 2 * D + p * 128:2 * D + (p + 1) * 128], causal)
            return 0

        lax.fori_loop(0, G // 2, self_rows, 0)
        need((3, 4), l, (5, 6, 7), 2)
        add_to_z(c_s, wo, l)
        norm_rows(z, n_s, MG)
        for n in range(0, D, TN):
            qkv[0:MG, n:n + TN] = jnp.dot(n_s[...], cq[l, :, n:n + TN], preferred_element_type=F32).astype(BF16)

        def cross_row(r, _):
            kv_wait(l, r)
            sl = lax.rem(r, 2)
            length = plan[P_LEN + first_row(i) + r]
            mask = lax.broadcasted_iota(I32, (two, T_ENC), 1) < length
            vmask = lax.broadcasted_iota(I32, (T_ENC, 128), 0) < length
            rows = pl.ds(pl.multiple_of(r * T_DEC, 32), T_DEC)
            for p in range(PAIRS):
                cols = slice(p * 128, (p + 1) * 128)
                c_s[rows, cols] = attend_pair(qkv[rows, cols], kb[sl, :, cols], vb[sl, :, cols], mask, vmask)

            @pl.when(r + 2 < G)
            def _():
                kv_start(l, r + 2)

            return 0

        lax.fori_loop(0, G, cross_row, 0)
        need((5, 6, 7), l, (0, 1, 2), 1)
        add_to_z(c_s, co, l)
        norm_rows(z, n_s, MG)
        for n in range(0, FF, TF):
            u = jnp.dot(n_s[...], w1[l, :, n:n + TF], preferred_element_type=F32)
            inner[:, n:n + TF] = gelu(u).astype(BF16)
        add_to_z(inner, w2, l)
        return 0

    lax.fori_loop(0, 2, layer, 0)

    for r in range(G):
        out_copy(i, slot, r).start()

    @pl.when(i == groups - 1)
    def _():
        for r in range(G):
            out_copy(i, slot, r).wait()


def decode_half(half, plan, y_dec, kvs, weights, prev):
    hbm = pl.BlockSpec(memory_space=pl.ANY)
    vm = lambda *s: pltpu.VMEM(s, BF16)
    ins = [y_dec, *kvs, *weights] + ([prev] if half else [])
    return pl.pallas_call(
        functools.partial(dec_kernel, half),
        out_shape=jax.ShapeDtypeStruct((ROWS, T_DEC, D), BF16),
        grid_spec=pltpu.PrefetchScalarGridSpec(
            num_scalar_prefetch=1,
            grid=(HALF // G,),
            in_specs=[hbm] * len(ins),
            out_specs=hbm,
            scratch_shapes=[
                vm(2, MG, D), vm(MG, D), vm(MG + 64, 3 * D), vm(MG, D),
                vm(2, T_ENC, D), vm(2, T_ENC, D),
                vm(2, D, D), vm(2, D, D), vm(2, D, D), vm(2, D, D), vm(2, D, D), vm(2, D, D), vm(2, D, FF), vm(2, FF, D),
                pltpu.SemaphoreType.DMA((2,)), pltpu.SemaphoreType.DMA((2,)), pltpu.SemaphoreType.DMA((2, 2)),
                pltpu.SemaphoreType.DMA((8, 2)),
            ],
        ),
        input_output_aliases={len(ins): 0} if half else {},
        compiler_params=pltpu.CompilerParams(vmem_limit_bytes=VMEM_MAX, dimension_semantics=("arbitrary",)),
        cost_estimate=pl.CostEstimate(flops=90_000_000_000, bytes_accessed=100_000_000, transcendentals=0),
        name="decode",
    )(plan, *ins)


def solution(mesh):
    pair_size = mesh.shape["pair"]
    to_partner = [(source, (source + pair_size // 2) % pair_size) for source in range(pair_size)]
    row_spec = P(("data", "pair"))
    full_spec = P()

    def per_device(x_enc, enc_len, y_dec, enc_wq, enc_wk, enc_wv, enc_wo, enc_w1, enc_w2, dec_wq, dec_wk, dec_wv, dec_wo, crs_wq, crs_wk, crs_wv, crs_wo, dec_w1, dec_w2):
        flat = lambda w: w.reshape(2, D, D)
        plan = make_plan(enc_len)
        partner_plan = lax.ppermute(plan, "pair", to_partner)
        enc_weights = (enc_wq, enc_wk, enc_wv, flat(enc_wo), enc_w1, enc_w2)
        enc_out, base, h = [], 0, x_enc
        for bins in CHUNKS:
            h = encode_chunk(base, bins, plan, x_enc, enc_weights, h)
            enc_out.append(lax.ppermute(h, "pair", to_partner))
            base += bins
        dec_weights = (dec_wq, dec_wk, dec_wv, flat(dec_wo), crs_wq, flat(crs_wo), dec_w1, dec_w2)
        out, kvs, after = None, [], h
        for half in range(2):
            hs = enc_out[2:] if half else enc_out[:2]
            kvs += cross_keys(half * NB // 2, partner_plan, hs, crs_wk, crs_wv, after)
            out = decode_half(half, partner_plan, y_dec, kvs, dec_weights, out)
            after = out
        return out

    return jax.shard_map(per_device, mesh=mesh, in_specs=(row_spec, row_spec, row_spec) + (full_spec,) * 16, out_specs=row_spec, check_vma=False)
```
